32 devices in a mesh: layer: 4 (over y, core), plane: 8 (over z, x).
Axes of the slice: x: 2, y: 2, z: 4, core: 2. Of those that a mesh axis runs over, the one named last changes fastest.
Arguments:
- polar: float32 [4, 512, 512], P('layer', 'plane'), may hold values from 0.1 to 1.6
- azimuth: float32 [4, 512, 512], P('layer', 'plane'), may hold values from -3 to 3
- saturation: float32 [4, 512, 512], P('layer', 'plane'), may hold values from 0.5 to 1.5
- anisotropy: float32 [4, 512, 512], P('layer', 'plane'), may hold values from 0.3 to 1.5
- stiffness: float32 [4], P('layer'), may hold values from 0.35 to 0.7
- coupling: float32 [3], replicated, may hold values from -1 to 1
Outputs:
- field: float32 [4, 3, 512, 512], P('layer', None, 'plane')
- moment: float32 [4, 3, 512, 512], P('layer', None, 'plane')
The draws below stay inside these ranges and needn't reach their ends.
All inputs are finite; a program needn't handle non-finite values.
Results may differ from the reference program's by a relative error of at most 0.00005.
Values sent between devices are 32-bit elements; how exact they have to be, the bound alone decides.
No kernel may reach another device: no remote copies, remote signals or barrier semaphores. Data moves between devices by JAX's collectives and lax.ppermute only.
A program may use at most 64 MiB of HBM per device.

```python
import math
import jax
import jax.numpy as jnp
from jax import lax

CELLS = 512
LAYERS = 4


def smooth_waves(key):
    first_key, second_key, phase_key = jax.random.split(key, 3)
    along_x = jax.random.randint(first_key, (LAYERS, 2), 1, 5)
    along_y = jax.random.randint(second_key, (LAYERS, 2), -4, 5)
    offset = jax.random.uniform(phase_key, (LAYERS, 2), jnp.float32, 0.0, 2.0 * jnp.pi)
    place = jnp.arange(CELLS, dtype=jnp.int32)
    turns = (along_x[:, :, None, None] * place[None, None, :, None] + along_y[:, :, None, None] * place[None, None, None, :]) % CELLS
    angle = turns.astype(jnp.float32) * (2.0 * jnp.pi / CELLS) + offset[:, :, None, None]
    waves = jnp.cos(angle)
    return 0.7 * waves[:, 0] + 0.3 * waves[:, 1]


def shared_wave(key):
    cycles = 183 * CELLS // 512
    place = jnp.arange(CELLS, dtype=jnp.int32)
    turns = cycles * place % CELLS
    offset = jax.random.uniform(key, (), jnp.float32, 0.0, 2.0 * jnp.pi)
    angle = turns.astype(jnp.float32) * (2.0 * jnp.pi / CELLS) + offset
    return jnp.cos(angle)[None, :, None]


def draw_polar(key, part):
    smooth = smooth_waves(jax.random.fold_in(key, 11))
    rough = jax.random.uniform(jax.random.fold_in(key, 12), (LAYERS, CELLS, CELLS), jnp.float32, -1.0, 1.0)
    common = shared_wave(jax.random.fold_in(key, 13))
    return 0.85 + 0.5 * common + 0.15 * smooth + 0.1 * rough


def draw_azimuth(key, part):
    smooth = smooth_waves(jax.random.fold_in(key, 21))
    rough = jax.random.uniform(jax.random.fold_in(key, 22), (LAYERS, CELLS, CELLS), jnp.float32, -1.0, 1.0)
    return 2.2 * smooth + 0.8 * rough


def steps_of(own_key, extent, cuts, low, largest):
    loudness = 1.0
    for dim, parts in cuts:
        heights = jax.random.uniform(jax.random.fold_in(jax.random.fold_in(own_key, 6), dim), (parts,), jnp.float32, low / len(cuts), largest / len(cuts))
        loudness = loudness * jnp.repeat(jnp.exp(heights), extent[dim] // parts).reshape((-1,) + (1,) * (len(extent) - 1 - dim))
    return loudness


def setup_inputs(seed: int = 0) -> dict:
    key_of = jax.random.split(jax.random.key(seed), 7)
    return {
        "polar": draw_polar(jax.random.fold_in(key_of[6], 71), 0),
        "azimuth": draw_azimuth(jax.random.fold_in(key_of[6], 71), 0),
        "saturation": jnp.clip(jnp.exp(math.log(1.5) - 1.0986123 * jax.random.uniform(key_of[2], (LAYERS, CELLS, CELLS), jnp.float32) ** steps_of(key_of[2], (LAYERS, CELLS, CELLS), ((0, 4), (1, 8)), -0.2, 0.2)), 0.5, 1.5),
        "anisotropy": jnp.clip(jnp.exp(math.log(1.5) - 1.60943787 * jax.random.uniform(key_of[3], (LAYERS, CELLS, CELLS), jnp.float32) ** steps_of(key_of[3], (LAYERS, CELLS, CELLS), ((0, 4), (1, 8)), -0.2, 0.2)), 0.3, 1.5),
        "stiffness": jnp.clip(jnp.exp(math.log(0.7) - 0.6931472 * jax.random.uniform(key_of[4], (LAYERS,), jnp.float32) ** steps_of(key_of[4], (LAYERS,), ((0, 4),), -0.2, 0.2)), 0.35, 0.7),
        "coupling": jnp.clip(jax.random.uniform(key_of[5], (LAYERS - 1,), jnp.float32, -1.0, 1.0), -1.0, 1.0),
    }


side_length = 512.0
spacing = 1.2
damping = 0.1
time_step = 0.1

def reference(polar, azimuth, saturation, anisotropy, stiffness, coupling):
    unit_moment = jnp.stack([jnp.sin(polar) * jnp.cos(azimuth), jnp.sin(polar) * jnp.sin(azimuth), jnp.cos(polar)], 1)
    magnet = unit_moment * saturation[:, None]
    pad_length = 2 * CELLS
    spectrum = jnp.fft.fft2(magnet, s=(pad_length, pad_length))
    wave_index = jnp.arange(pad_length, dtype=jnp.int32)
    folded = jnp.where(wave_index < CELLS, wave_index, wave_index - pad_length)
    wavenumber = jnp.pi * folded.astype(jnp.float32) / side_length
    wave_x = wavenumber[:, None]
    wave_y = wavenumber[None, :]
    magnitude = jnp.sqrt(wave_x * wave_x + wave_y * wave_y)
    nonzero = magnitude > 0.0
    safe = jnp.where(nonzero, magnitude, 1.0)
    unit_x = jnp.where(nonzero, wave_x / safe, 0.0)
    unit_y = jnp.where(nonzero, wave_y / safe, 0.0)
    self_part = jnp.where(nonzero, -jnp.expm1(-safe) / safe, 1.0)
    half_sinh = jnp.sinh(0.5 * safe)
    mutual = jnp.where(nonzero, 2.0 * half_sinh * half_sinh / safe, 0.0)
    decay = jnp.exp(-spacing * magnitude)
    inplane = unit_x * spectrum[:, 0] + unit_y * spectrum[:, 1]
    upward = spectrum[:, 2] - 1j * inplane
    downward = -spectrum[:, 2] - 1j * inplane
    carry = jnp.zeros_like(upward[0])
    below_list = []
    for layer_number in range(LAYERS):
        below_list.append(carry)
        carry = decay * (carry + upward[layer_number])
    carry = jnp.zeros_like(upward[0])
    above_list = [None] * LAYERS
    for layer_number in range(LAYERS - 1, -1, -1):
        above_list[layer_number] = carry
        carry = decay * (carry + downward[layer_number])
    below = jnp.stack(below_list)
    above = jnp.stack(above_list)
    total = below + above
    differ = below - above
    field_x = -(1.0 - self_part) * unit_x * inplane - 1j * unit_x * mutual * total
    field_y = -(1.0 - self_part) * unit_y * inplane - 1j * unit_y * mutual * total
    field_z = -self_part * spectrum[:, 2] + mutual * differ
    demag = jnp.real(jnp.fft.ifft2(jnp.stack([field_x, field_y, field_z], 1))[..., :CELLS, :CELLS])
    padded = jnp.pad(unit_moment, ((1, 1), (0, 0), (1, 1), (1, 1)))
    beside = padded[1:-1, :, :-2, 1:-1] + padded[1:-1, :, 2:, 1:-1]
    beside = beside + padded[1:-1, :, 1:-1, :-2] + padded[1:-1, :, 1:-1, 2:]
    nothing = jnp.zeros((1,), coupling.dtype)
    lower_link = jnp.concatenate([nothing, coupling])
    upper_link = jnp.concatenate([coupling, nothing])
    exchange = stiffness[:, None, None, None] * beside
    exchange = exchange + lower_link[:, None, None, None] * padded[:-2, :, 1:-1, 1:-1]
    exchange = exchange + upper_link[:, None, None, None] * padded[2:, :, 1:-1, 1:-1]
    zeros_plane = jnp.zeros_like(anisotropy)
    uniaxial = jnp.stack([zeros_plane, zeros_plane, anisotropy * unit_moment[:, 2]], 1)
    field = demag + exchange + uniaxial
    first_cross = jnp.cross(unit_moment, field, axis=1)
    second_cross = jnp.cross(unit_moment, first_cross, axis=1)
    torque = -(first_cross + damping * second_cross) / (1.0 + damping * damping)
    stepped = unit_moment + time_step * torque
    length = jnp.sqrt(lax.optimization_barrier(jnp.sum(stepped * stepped, axis=1, keepdims=True)))
    return (field, stepped / length)
```

```python
import functools
import math

import jax
import jax.numpy as jnp
import numpy as np
from jax import lax
from jax.experimental import pallas as pl
from jax.experimental.pallas import tpu as pltpu
from jax.sharding import PartitionSpec as P

side_length = 512.0
spacing = 1.2
damping = 0.1
time_step = 0.1
exact = lax.Precision.HIGHEST

lanes = 128
sublanes = 8
half = lanes // 2
root_half = math.sqrt(0.5)
chunk_count = 1
coef_count = 13
both = ("layer", "plane")
in_vmem = pl.BlockSpec(memory_space=pltpu.VMEM)
in_smem = pl.BlockSpec(memory_space=pltpu.SMEM)


def split_table(table):
    head = table.astype(np.float32).astype(jnp.bfloat16)
    rest = (table - head.astype(np.float64)).astype(np.float32).astype(jnp.bfloat16)
    return np.stack([head, rest])


def row_table(cell_count):
    turns = np.outer(np.arange(cell_count), np.arange(cell_count)) % (2 * cell_count)
    phase = turns * (np.pi / cell_count)
    return split_table(np.concatenate([np.cos(phase), -np.sin(phase)]))


def short_tables():
    turns = np.outer(np.arange(lanes), np.arange(lanes)) % lanes
    phase = turns * (2.0 * np.pi / lanes)
    c, s = np.cos(phase), np.sin(phase)
    return split_table(np.block([[c, -s], [s, c]])), split_table(np.block([[c, s], [-s, c]]))


def twiddle_table(radix):
    phase = np.outer(np.arange(radix), np.arange(lanes)) * (2.0 * np.pi / (radix * lanes))
    pair = np.stack([np.cos(phase), np.sin(phase)]).astype(np.float32)
    return np.ascontiguousarray(np.broadcast_to(pair[:, :, None], (2, radix, sublanes, lanes)))


def split(value):
    head = value.astype(jnp.bfloat16)
    return head, (value - head.astype(jnp.float32)).astype(jnp.bfloat16)


def product(left, right, dims):
    dot = functools.partial(
        lax.dot_general, dimension_numbers=(dims, ((), ())), preferred_element_type=jnp.float32
    )
    return dot(left[0], right[0]) + (dot(left[1], right[0]) + dot(left[0], right[1]))


def sine_cosine(angle):
    square = angle * angle
    sine = jnp.full_like(angle, 1.0 / math.factorial(13))
    for order in (11, 9, 7, 5, 3, 1):
        sine = (-1.0) ** ((order - 1) // 2) / math.factorial(order) + square * sine
    cosine = jnp.full_like(angle, -1.0 / math.factorial(14))
    for order in (12, 10, 8, 6, 4, 2, 0):
        cosine = (-1.0) ** (order // 2) / math.factorial(order) + square * cosine
    return angle * sine, cosine


def first_kernel(polar_ref, azimuth_ref, saturation_ref, table_ref, moment_ref, head_ref, tail_ref, *out_refs):
    rows, cell_count = polar_ref.shape
    sin_polar, cos_polar = sine_cosine(polar_ref[...])
    sin_half, cos_half = sine_cosine(0.5 * azimuth_ref[...])
    moment = (
        sin_polar * (1.0 - 2.0 * sin_half * sin_half),
        sin_polar * (2.0 * sin_half * cos_half),
        cos_polar,
    )
    for c in range(3):
        moment_ref[c] = moment[c]
        head_ref[c : c + 1] = moment[c][:1]
        tail_ref[c : c + 1] = moment[c][rows - 1 :]
    saturation = saturation_ref[...]
    magnet = [split(m * saturation) for m in moment]
    blank = jnp.zeros((rows, cell_count), jnp.bfloat16)
    for_real = [jnp.concatenate([m[n] for m in magnet] + [blank]) for n in range(2)]
    for_imag = [jnp.concatenate([blank] + [m[n] for m in magnet]) for n in range(2)]
    dims = ((1,), (1,))
    span = cell_count // len(out_refs)
    for n, out_ref in enumerate(out_refs):
        start = n * span
        cosine = (table_ref[0, start : start + span], table_ref[1, start : start + span])
        start += cell_count
        sine = (table_ref[0, start : start + span], table_ref[1, start : start + span])
        real = product(cosine, for_real, dims)
        imag = product(sine, for_imag, dims)
        out_ref[:, :lanes] = real[:, :lanes]
        out_ref[:, lanes : 2 * lanes] = real[:, lanes:] + imag[:, :lanes]
        out_ref[:, 2 * lanes :] = imag[:, lanes:]


def factors(wave_x, wave_y):
    magnitude = jnp.sqrt(wave_x * wave_x + wave_y * wave_y)
    nonzero = magnitude > 0.0
    safe = jnp.where(nonzero, magnitude, 1.0)
    inverse = 1.0 / safe
    series = jnp.ones_like(safe)
    for order in range(9, 1, -1):
        series = 1.0 - series * safe * (1.0 / order)
    growth = jnp.exp(safe)
    lost = jnp.where(safe < 0.5, series * safe, 1.0 - jnp.exp(-safe))
    self_part = jnp.where(nonzero, lost * inverse, 1.0)
    mutual = jnp.where(nonzero, lost * lost * growth * (0.5 * inverse), 0.0)
    decay = jnp.exp(-spacing * magnitude)
    unit_x = jnp.where(nonzero, wave_x * inverse, 0.0)
    unit_y = jnp.where(nonzero, wave_y * inverse, 0.0)
    return unit_x, unit_y, self_part, mutual, decay


def coef_kernel(base_ref, *out_refs, cell_count, span):
    pad_length = 2 * cell_count
    radix = pad_length // lanes
    step = math.pi / side_length
    for n, out_ref in enumerate(out_refs):
        slots = out_ref.shape[2]
        shape = (slots, lanes)
        slot = n * span + base_ref[0] * slots + lax.broadcasted_iota(jnp.int32, shape, 0)
        wave_y = step * slot.astype(jnp.float32)
        weight = jnp.where(slot == 0, 1.0, 2.0) / float(pad_length * pad_length)
        signed = jnp.where(slot % 2 == 0, weight, -weight)
        for r in range(radix):
            index = lax.broadcasted_iota(jnp.int32, shape, 1) * radix + r
            middle = index == cell_count
            folded = jnp.where(index < cell_count, index, index - pad_length)
            wave_x = step * folded.astype(jnp.float32)
            unit_x, unit_y, self_part, mutual, decay = factors(wave_x, wave_y)
            out_ref[0, r] = jnp.where(middle, 0.0, unit_x)
            out_ref[1, r] = unit_y
            out_ref[2, r] = (1.0 - self_part) * weight
            out_ref[3, r] = self_part * weight
            out_ref[4, r] = mutual * weight
            out_ref[5, r] = decay
            edge = jnp.full(shape, -step * cell_count, jnp.float32)
            edge_x, edge_y, self_part, mutual, decay = factors(wave_x, edge)
            rest = (1.0 - self_part) * signed
            mutual = mutual * signed
            square = edge_y * edge_y
            out_ref[6, r] = jnp.where(middle, 0.0, edge_x)
            out_ref[7, r] = rest
            out_ref[8, r] = self_part * signed
            out_ref[9, r] = mutual
            out_ref[10, r] = decay
            out_ref[11, r] = rest * square
            out_ref[12, r] = mutual * square


def neighbours(values, decay):
    count = len(values)
    under = [None] * count
    over = [None] * count
    for t in range(1, count):
        under[t] = decay * (values[t - 1] if under[t - 1] is None else under[t - 1] + values[t - 1])
    for t in range(count - 2, -1, -1):
        over[t] = decay * (values[t + 1] if over[t + 1] is None else over[t + 1] + values[t + 1])
    return under, over


def joined(first, second, sign=1.0):
    if first is None:
        return second if sign > 0.0 else -second
    if second is None:
        return first
    return first + second if sign > 0.0 else first - second


def drive(x, z, keep, mutual, decay, own):
    count = len(x)
    up_r, over_r = [z[t][0] + x[t][1] for t in range(count)], [x[t][1] - z[t][0] for t in range(count)]
    up_i, over_i = [z[t][1] - x[t][0] for t in range(count)], [-z[t][1] - x[t][0] for t in range(count)]
    below_r, below_i = neighbours(up_r, decay)[0], neighbours(up_i, decay)[0]
    above_r, above_i = neighbours(over_r, decay)[1], neighbours(over_i, decay)[1]
    inner, outer = [], []
    for t in range(count):
        total_r, total_i = joined(below_r[t], above_r[t]), joined(below_i[t], above_i[t])
        differ_r = joined(below_r[t], above_r[t], -1.0)
        differ_i = joined(below_i[t], above_i[t], -1.0)
        inner.append((mutual * total_i - keep * x[t][0], -(mutual * total_r) - keep * x[t][1]))
        outer.append((mutual * differ_r - own * z[t][0], mutual * differ_i - own * z[t][1]))
    return inner, outer


def even_part(values, keep, mutual, decay):
    out = []
    for n in range(2):
        part = [v[n] for v in values]
        under, over = neighbours(part, decay)
        out.append([-(keep * part[t]) - mutual * joined(under[t], over[t]) for t in range(len(part))])
    return list(zip(*out))


def respond(spectrum, coef, has_middle, middle):
    count = len(spectrum)
    unit_x, unit_y, keep, own, mutual, decay = coef[:6]
    edge_x, edge_keep, edge_own, edge_mutual, edge_decay, keep_y, mutual_y = coef[6:]
    x = [s[0] for s in spectrum]
    y = [s[1] for s in spectrum]
    z = [s[2] for s in spectrum]
    charge = [tuple(unit_x * x[t][n] + unit_y * y[t][n] for n in range(2)) for t in range(count)]
    inner, outer = drive(charge, z, keep, mutual, decay, own)
    charge = [tuple(edge_x * x[t][n] for n in range(2)) for t in range(count)]
    edge_inner, edge_outer = drive(charge, z, edge_keep, edge_mutual, edge_decay, edge_own)
    edge_y = even_part(y, keep_y, mutual_y, edge_decay)
    out = []
    for t in range(count):
        out.append(
            [
                tuple(unit_x * inner[t][n] - edge_x * edge_inner[t][n] for n in range(2)),
                tuple(unit_y * inner[t][n] - edge_y[t][n] for n in range(2)),
                tuple(outer[t][n] - edge_outer[t][n] for n in range(2)),
            ]
        )
    if has_middle:
        square = jnp.where(middle, 1.0 - unit_y * unit_y, 0.0)
        alone = even_part(x, keep * square, mutual * square, decay)
        keep_m, mutual_m = jnp.where(middle, keep_y, 0.0), jnp.where(middle, mutual_y, 0.0)
        cross_x = even_part(x, keep_m, mutual_m, edge_decay)
        cross_y = even_part(y, keep_m, mutual_m, edge_decay)
        for t in range(count):
            out[t][0] = tuple(
                out[t][0][n] + alone[t][n] - cross_x[t][n] - cross_y[t][n] for n in range(2)
            )
            out[t][1] = tuple(out[t][1][n] - cross_x[t][n] for n in range(2))
    return out


def add(a, b):
    return a[0] + b[0], a[1] + b[1]


def sub(a, b):
    return a[0] - b[0], a[1] - b[1]


def add_turned(a, b):
    return a[0] - b[1], a[1] + b[0]


def sub_turned(a, b):
    return a[0] + b[1], a[1] - b[0]


def four_point(z):
    s, d, u, v = add(z[0], z[2]), sub(z[0], z[2]), add(z[1], z[3]), sub(z[1], z[3])
    return add(s, u), sub_turned(d, v), sub(s, u), add_turned(d, v)


def four_point_back(z):
    s, d, u, v = add(z[0], z[2]), sub(z[0], z[2]), add(z[1], z[3]), sub(z[1], z[3])
    return add(s, u), add_turned(d, v), sub(s, u), sub_turned(d, v)


def spread(z):
    turned = [
        z[0],
        (root_half * (z[1][0] + z[1][1]), root_half * (z[1][1] - z[1][0])),
        (z[2][1], -z[2][0]),
        (root_half * (z[3][1] - z[3][0]), -root_half * (z[3][0] + z[3][1])),
    ]
    even, odd = four_point(z), four_point(turned)
    return [even[r // 2] if r % 2 == 0 else odd[r // 2] for r in range(8)]


def gather_back(v):
    even, odd = four_point_back(v[0::2]), four_point_back(v[1::2])
    return [
        add(even[0], odd[0]),
        (even[1][0] + root_half * (odd[1][0] - odd[1][1]), even[1][1] + root_half * (odd[1][0] + odd[1][1])),
        add_turned(even[2], odd[2]),
        (even[3][0] - root_half * (odd[3][0] + odd[3][1]), even[3][1] + root_half * (odd[3][0] - odd[3][1])),
    ]


def middle_kernel(rows_ref, coef_ref, twiddle_ref, forward_ref, back_ref, out_ref, work_ref, *, layers):
    radix = twiddle_ref.shape[1]
    pieces = radix // 2
    planes = rows_ref.shape[0] // layers
    items = layers * 3
    place = lax.broadcasted_iota(jnp.int32, (sublanes, lanes), 1)
    low = place < half

    def piece(row, part):
        tile, upper = divmod(part, 2)
        cut = slice(tile * lanes, (tile + 1) * lanes)
        first, second = rows_ref[row, :, cut], rows_ref[row + 1, :, cut]
        if upper:
            return jnp.where(low, pltpu.roll(first, half, 1), second)
        return jnp.where(low, first, pltpu.roll(second, half, 1))

    for item in range(items):
        layer, c = divmod(item, 3)
        z = [
            (piece(layer * planes + 2 * p, c), piece(layer * planes + 2 * p, 3 + c)) for p in range(pieces)
        ]
        for r, (real, imag) in enumerate(spread(z)):
            if r > 0:
                cosine, sine = twiddle_ref[0, r], twiddle_ref[1, r]
                real, imag = real * cosine + imag * sine, imag * cosine - real * sine
            start = item * sublanes
            work_ref[r, start : start + sublanes, :lanes] = real
            work_ref[r, start : start + sublanes, lanes:] = imag
    dims = ((1,), (0,))
    forward = (forward_ref[0], forward_ref[1])
    back = (back_ref[0], back_ref[1])
    for r in range(radix):
        value = product(split(work_ref[r]), forward, dims)
        spectrum = [
            [
                (
                    value[(t * 3 + c) * sublanes : (t * 3 + c + 1) * sublanes, :lanes],
                    value[(t * 3 + c) * sublanes : (t * 3 + c + 1) * sublanes, lanes:],
                )
                for c in range(3)
            ]
            for t in range(layers)
        ]
        coef = [coef_ref[n, r] for n in range(coef_count)]
        out = respond(spectrum, coef, r == 0, place * radix + r == radix * half)
        value = jnp.concatenate(
            [jnp.concatenate([pair[0], pair[1]], axis=1) for layer in out for pair in layer]
        )
        work_ref[r] = product(split(value), back, dims)
    for layer in range(layers):
        parts = [[None] * 6 for _ in range(pieces)]
        for c in range(3):
            start = (layer * 3 + c) * sublanes
            v = []
            for r in range(radix):
                real = work_ref[r, start : start + sublanes, :lanes]
                imag = work_ref[r, start : start + sublanes, lanes:]
                if r > 0:
                    cosine, sine = twiddle_ref[0, r], twiddle_ref[1, r]
                    real, imag = real * cosine - imag * sine, imag * cosine + real * sine
                v.append((real, imag))
            for p, (real, imag) in enumerate(gather_back(v)):
                parts[p][c], parts[p][3 + c] = real, imag
        for p in range(pieces):
            row = layer * planes + 2 * p
            for tile in range(3):
                first, second = parts[p][2 * tile], parts[p][2 * tile + 1]
                cut = slice(tile * lanes, (tile + 1) * lanes)
                out_ref[row, :, cut] = jnp.where(low, first, pltpu.roll(second, half, 1))
                out_ref[row + 1, :, cut] = jnp.where(low, pltpu.roll(first, half, 1), second)


def exchange_kernel(link_ref, moment_ref, below_ref, above_ref, before_ref, after_ref, anisotropy_ref, out_ref):
    rows, cell_count = anisotropy_ref.shape
    row = lax.broadcasted_iota(jnp.int32, (rows, cell_count), 0)
    column = lax.broadcasted_iota(jnp.int32, (rows, cell_count), 1)
    stiffness, lower_link, upper_link = link_ref[0], link_ref[1], link_ref[2]
    for c in range(3):
        m = moment_ref[c]
        before = jnp.where(row == 0, before_ref[c : c + 1], pltpu.roll(m, 1, 0))
        after = jnp.where(row == rows - 1, after_ref[c : c + 1], pltpu.roll(m, rows - 1, 0))
        left = jnp.where(column == 0, 0.0, pltpu.roll(m, 1, 1))
        right = jnp.where(column == cell_count - 1, 0.0, pltpu.roll(m, cell_count - 1, 1))
        total = stiffness * (before + after + left + right)
        total = total + lower_link * below_ref[c] + upper_link * above_ref[c]
        if c == 2:
            total = total + anisotropy_ref[...] * m
        out_ref[c] = total


def inverse_rows(block_refs, table_ref, cell_count, rows):
    span = cell_count // len(block_refs)
    dims = ((1,), (0,))
    total = None
    for n, block_ref in enumerate(block_refs):
        turned = block_ref[...].T
        for part in range(2):
            start = part * cell_count + n * span
            table = (table_ref[0, start : start + span], table_ref[1, start : start + span])
            term = product(split(turned[part * 3 * rows : (part + 1) * 3 * rows]), table, dims)
            total = term if total is None else total + term
    return total


def last_kernel(moment_ref, other_ref, table_ref, *refs):
    block_refs, (field_ref, out_ref) = refs[:-2], refs[-2:]
    rows, cell_count = moment_ref.shape[1:]
    demag = inverse_rows(block_refs, table_ref, cell_count, rows)
    m = [moment_ref[c] for c in range(3)]
    f = [other_ref[c] + demag[c * rows : (c + 1) * rows] for c in range(3)]
    first = cross(m, f)
    second = cross(m, first)
    stepped = []
    for c in range(3):
        field_ref[c] = f[c]
        torque = -(first[c] + damping * second[c]) / (1.0 + damping * damping)
        stepped.append(m[c] + time_step * torque)
    scale = lax.rsqrt(stepped[0] * stepped[0] + stepped[1] * stepped[1] + stepped[2] * stepped[2])
    for c in range(3):
        out_ref[c] = stepped[c] * scale


def cross(first, second):
    return [
        first[1] * second[2] - first[2] * second[1],
        first[2] * second[0] - first[0] * second[2],
        first[0] * second[1] - first[1] * second[0],
    ]


def shift(value, axis, step):
    count = lax.axis_size(axis)
    pairs = [(i, i + step) for i in range(count) if 0 <= i + step < count]
    return lax.ppermute(value, axis, pairs)


def fast_body(polar, azimuth, saturation, anisotropy, stiffness, coupling):
    rows, cell_count = polar.shape[1:]
    layers, planes = lax.axis_size("layer"), lax.axis_size("plane")
    device_count = layers * planes
    layer_index = lax.axis_index("layer")
    plane_index = lax.axis_index("plane")
    span = cell_count // chunk_count
    slots = span // device_count
    radix = 2 * cell_count // lanes
    width = 6 * rows
    f32 = jnp.float32
    table = jnp.asarray(row_table(cell_count))
    forward, back = (jnp.asarray(t) for t in short_tables())
    twiddle = jnp.asarray(twiddle_table(radix))

    moment, top, bottom, *sent = pl.pallas_call(
        first_kernel,
        out_shape=[
            jax.ShapeDtypeStruct((3, rows, cell_count), f32),
            jax.ShapeDtypeStruct((sublanes, cell_count), f32),
            jax.ShapeDtypeStruct((sublanes, cell_count), f32),
        ]
        + [jax.ShapeDtypeStruct((span, width), f32)] * chunk_count,
        in_specs=[in_vmem] * 4,
        out_specs=[in_vmem] * (3 + chunk_count),
        cost_estimate=pl.CostEstimate(
            flops=12 * rows * cell_count * cell_count * 6, bytes_accessed=8 << 20, transcendentals=0
        ),
        name="first",
    )(polar[0], azimuth[0], saturation[0], table)

    base = (layer_index * planes + plane_index).astype(jnp.int32).reshape(1)
    coefs = pl.pallas_call(
        functools.partial(coef_kernel, cell_count=cell_count, span=span),
        out_shape=[jax.ShapeDtypeStruct((coef_count, radix, slots, lanes), f32)] * chunk_count,
        in_specs=[in_smem],
        out_specs=[in_vmem] * chunk_count,
        cost_estimate=pl.CostEstimate(flops=20 << 20, bytes_accessed=1 << 20, transcendentals=1 << 16),
        name="coefs",
    )(base)

    below = shift(moment, "layer", 1)
    above = shift(moment, "layer", -1)
    before = shift(bottom, "plane", 1)
    after = shift(top, "plane", -1)
    links = jnp.stack(
        [
            stiffness[0],
            coupling[jnp.maximum(layer_index - 1, 0)],
            coupling[jnp.minimum(layer_index, coupling.shape[0] - 1)],
        ]
    )
    other = pl.pallas_call(
        exchange_kernel,
        out_shape=jax.ShapeDtypeStruct((3, rows, cell_count), f32),
        in_specs=[in_smem] + [in_vmem] * 6,
        out_specs=in_vmem,
        cost_estimate=pl.CostEstimate(flops=20 << 20, bytes_accessed=2 << 20, transcendentals=0),
        name="exchange",
    )(links, moment, below, above, before, after, anisotropy[0])

    received = []
    for n in range(chunk_count):
        block = sent[n].reshape(device_count, slots, width)
        block = lax.all_to_all(block, both, split_axis=0, concat_axis=0, tiled=True)
        block = pl.pallas_call(
            functools.partial(middle_kernel, layers=layers),
            grid=(slots // sublanes,),
            out_shape=jax.ShapeDtypeStruct((device_count, slots, width), f32),
            in_specs=[
                pl.BlockSpec((device_count, sublanes, width), lambda g: (0, g, 0)),
                pl.BlockSpec((coef_count, radix, sublanes, lanes), lambda g: (0, 0, g, 0)),
                pl.BlockSpec((2, radix, sublanes, lanes), lambda g: (0, 0, 0, 0)),
                pl.BlockSpec((2, 2 * lanes, 2 * lanes), lambda g: (0, 0, 0)),
                pl.BlockSpec((2, 2 * lanes, 2 * lanes), lambda g: (0, 0, 0)),
            ],
            out_specs=pl.BlockSpec((device_count, sublanes, width), lambda g: (0, g, 0)),
            scratch_shapes=[pltpu.VMEM((radix, layers * 3 * sublanes, 2 * lanes), f32)],
            cost_estimate=pl.CostEstimate(flops=2000 << 20, bytes_accessed=4 << 20, transcendentals=0),
            name="middle",
        )(block, coefs[n], twiddle, forward, back)
        block = lax.all_to_all(block, both, split_axis=0, concat_axis=0, tiled=True)
        received.append(block.reshape(span, width))

    field, stepped = pl.pallas_call(
        last_kernel,
        out_shape=[jax.ShapeDtypeStruct((3, rows, cell_count), f32)] * 2,
        in_specs=[in_vmem] * (3 + chunk_count),
        out_specs=[in_vmem] * 2,
        cost_estimate=pl.CostEstimate(
            flops=12 * rows * cell_count * cell_count * 6, bytes_accessed=8 << 20, transcendentals=0
        ),
        name="last",
    )(moment, other, table, *received)
    return field[None], stepped[None]


def with_halo(cells, sides, width):
    for axis, dim in sides:
        count = lax.axis_size(axis)
        ends = count - 1
        head = lax.slice_in_dim(cells, 0, width, axis=dim)
        tail = lax.slice_in_dim(cells, cells.shape[dim] - width, cells.shape[dim], axis=dim)
        cells = jnp.concatenate(
            [
                lax.ppermute(tail, axis, [(i, (i + 1) % count) for i in range(ends)]),
                cells,
                lax.ppermute(head, axis, [((i + 1) % count, i) for i in range(ends)]),
            ],
            axis=dim,
        )
    return cells


def cross_product(first, second):
    return jnp.stack(
        [
            first[1] * second[2] - first[2] * second[1],
            first[2] * second[0] - first[0] * second[2],
            first[0] * second[1] - first[1] * second[0],
        ]
    )


def signed_wave(index, cell_count):
    folded = jnp.where(index < cell_count, index, index - 2 * cell_count)
    return jnp.pi * folded.astype(jnp.float32) / side_length


def plain_body(polar, azimuth, saturation, anisotropy, stiffness, coupling):
    row_count = polar.shape[1]
    cell_count = polar.shape[2]
    pad_length = 2 * cell_count
    plane_count = lax.axis_size("plane")
    band_width = pad_length // plane_count
    layer_index = lax.axis_index("layer")
    plane_index = lax.axis_index("plane")
    theta = polar[0]
    azimuthal = azimuth[0]
    moment_in = jnp.stack(
        [jnp.sin(theta) * jnp.cos(azimuthal), jnp.sin(theta) * jnp.sin(azimuthal), jnp.cos(theta)]
    )
    magnet = moment_in * saturation[0][None]
    place = jnp.arange(cell_count, dtype=jnp.int32)
    wave_index = jnp.arange(pad_length, dtype=jnp.int32)
    turns = place[:, None] * wave_index[None, :] % pad_length
    phase = turns.astype(jnp.float32) * (2.0 * jnp.pi / pad_length)
    cosine = jnp.cos(phase)
    sine = jnp.sin(phase)
    cosine_blocks = cosine.reshape(plane_count, row_count, pad_length)
    sine_blocks = sine.reshape(plane_count, row_count, pad_length)
    cosine_bands = cosine.reshape(cell_count, plane_count, band_width)
    sine_bands = sine.reshape(cell_count, plane_count, band_width)
    along_real = jnp.einsum("cxy,yk->ckx", magnet, cosine, precision=exact)
    along_imag = -jnp.einsum("cxy,yk->ckx", magnet, sine, precision=exact)
    sectioned = jnp.stack([along_real, along_imag], 1).reshape(
        3, 2, plane_count, band_width * row_count
    )
    block = lax.all_to_all(sectioned, "plane", split_axis=2, concat_axis=2, tiled=True)
    item_count = block.shape[0]
    split = block.reshape(item_count, 2, plane_count, band_width, row_count)
    with_cosine = jnp.einsum("npsqx,sxk->npqk", split, cosine_blocks, precision=exact)
    with_sine = jnp.einsum("npsqx,sxk->npqk", split, sine_blocks, precision=exact)
    spectrum = jnp.stack(
        [with_cosine[:, 0] + with_sine[:, 1], with_cosine[:, 1] - with_sine[:, 0]], 1
    )
    wave_y = signed_wave(
        plane_index * band_width + jnp.arange(band_width, dtype=jnp.int32), cell_count
    )[:, None]
    wave_x = signed_wave(wave_index, cell_count)[None, :]
    magnitude = jnp.sqrt(wave_x * wave_x + wave_y * wave_y)
    nonzero = magnitude > 0.0
    safe = jnp.where(nonzero, magnitude, 1.0)
    unit_x = jnp.where(nonzero, wave_x / safe, 0.0)
    unit_y = jnp.where(nonzero, wave_y / safe, 0.0)
    self_part = jnp.where(nonzero, -jnp.expm1(-safe) / safe, 1.0)
    half_sinh = jnp.sinh(0.5 * safe)
    mutual = jnp.where(nonzero, 2.0 * half_sinh * half_sinh / safe, 0.0)
    spectral_x = spectrum[0]
    spectral_y = spectrum[1]
    spectral_z = spectrum[2]
    inplane = unit_x * spectral_x + unit_y * spectral_y
    upward = jnp.stack([spectral_z[0] + inplane[1], spectral_z[1] - inplane[0]])
    downward = jnp.stack([-spectral_z[0] + inplane[1], -spectral_z[1] - inplane[0]])
    emitted = jnp.stack([upward, downward])[None]
    piece = lax.all_gather(emitted, "layer", axis=0, tiled=True)
    source = jnp.arange(piece.shape[0], dtype=jnp.int32)
    separation = layer_index - source
    distance = jnp.abs(separation).astype(jnp.float32)
    weight = jnp.exp(-spacing * distance[:, None, None] * magnitude[None])
    lower = jnp.where((separation > 0)[:, None, None], weight, 0.0)
    upper = jnp.where((separation < 0)[:, None, None], weight, 0.0)
    below = jnp.sum(lower[:, None] * piece[:, 0], 0)
    above = jnp.sum(upper[:, None] * piece[:, 1], 0)
    total = below + above
    differ = below - above
    remainder = 1.0 - self_part
    field_x = jnp.stack(
        [
            -remainder * unit_x * inplane[0] + unit_x * mutual * total[1],
            -remainder * unit_x * inplane[1] - unit_x * mutual * total[0],
        ]
    )
    field_y = jnp.stack(
        [
            -remainder * unit_y * inplane[0] + unit_y * mutual * total[1],
            -remainder * unit_y * inplane[1] - unit_y * mutual * total[0],
        ]
    )
    field_z = jnp.stack(
        [
            -self_part * spectral_z[0] + mutual * differ[0],
            -self_part * spectral_z[1] + mutual * differ[1],
        ]
    )
    spectral = jnp.stack([field_x, field_y, field_z])
    back_cosine = jnp.einsum("cpqk,sxk->cpsqx", spectral, cosine_blocks, precision=exact)
    back_sine = jnp.einsum("cpqk,sxk->cpsqx", spectral, sine_blocks, precision=exact)
    returned = jnp.stack(
        [back_cosine[:, 0] - back_sine[:, 1], back_sine[:, 0] + back_cosine[:, 1]], 1
    )
    returned = returned.reshape(3, 2, plane_count, band_width * row_count)
    scale = 1.0 / (float(pad_length) * float(pad_length))
    block = lax.all_to_all(returned, "plane", split_axis=2, concat_axis=2, tiled=True)
    item_count = block.shape[0]
    split = block.reshape(item_count, 2, plane_count, band_width, row_count)
    real_part = jnp.einsum("nsqx,ysq->nxy", split[:, 0], cosine_bands, precision=exact)
    imag_part = jnp.einsum("nsqx,ysq->nxy", split[:, 1], sine_bands, precision=exact)
    demag = (real_part - imag_part) * scale
    padded = with_halo(moment_in[None], (("layer", 0), ("plane", 2)), 1)
    centre = padded[1]
    beside = centre[:, :-2] + centre[:, 2:]
    sideways = jnp.pad(moment_in, ((0, 0), (0, 0), (1, 1)))
    beside = beside + sideways[:, :, :-2] + sideways[:, :, 2:]
    lower_link = coupling[jnp.maximum(layer_index - 1, 0)]
    upper_link = coupling[jnp.minimum(layer_index, coupling.shape[0] - 1)]
    exchange_field = (
        stiffness[0] * beside + lower_link * padded[0, :, 1:-1] + upper_link * padded[2, :, 1:-1]
    )
    flat_zero = jnp.zeros_like(moment_in[2])
    uniaxial = jnp.stack([flat_zero, flat_zero, anisotropy[0] * moment_in[2]])
    field = demag + exchange_field + uniaxial
    first_cross = cross_product(moment_in, field)
    second_cross = cross_product(moment_in, first_cross)
    torque = -(first_cross + damping * second_cross) / (1.0 + damping * damping)
    stepped = moment_in + time_step * torque
    length = jnp.sqrt(jnp.sum(stepped * stepped, axis=0, keepdims=True))
    return (field[None], (stepped / length)[None])


def body(polar, azimuth, saturation, anisotropy, stiffness, coupling):
    rows, cell_count = polar.shape[1:]
    device_count = lax.axis_size("layer") * lax.axis_size("plane")
    fits = 2 * rows == lanes and cell_count == 4 * lanes
    fits = fits and cell_count % (chunk_count * device_count * sublanes) == 0
    chosen = fast_body if fits else plain_body
    return chosen(polar, azimuth, saturation, anisotropy, stiffness, coupling)


def solution(mesh):
    placed = (
        P("layer", "plane", None),
        P("layer", "plane", None),
        P("layer", "plane", None),
        P("layer", "plane", None),
        P("layer"),
        P(),
    )
    return jax.shard_map(
        body,
        mesh=mesh,
        in_specs=placed,
        out_specs=(P("layer", None, "plane", None), P("layer", None, "plane", None)),
        check_vma=False,
    )
```

```python
import functools
import math

import jax
import jax.numpy as jnp
import numpy as np
from jax import lax
from jax.experimental import pallas as pl
from jax.experimental.pallas import tpu as pltpu
from jax.sharding import PartitionSpec as P

side_length = 512.0
spacing = 1.2
damping = 0.1
time_step = 0.1
exact = lax.Precision.HIGHEST

lanes = 128
sublanes = 8
half = lanes // 2
root_half = math.sqrt(0.5)
piece_count = 4
coef_count = 13
vmem_limit = 16 << 20
both = ("plane", "layer")
in_vmem = pl.BlockSpec(memory_space=pltpu.VMEM)
in_any = pl.BlockSpec(memory_space=pl.ANY)
in_smem = pl.BlockSpec(memory_space=pltpu.SMEM)


def split_table(table):
    head = table.astype(np.float32).astype(jnp.bfloat16)
    rest = (table - head.astype(np.float64)).astype(np.float32).astype(jnp.bfloat16)
    return np.stack([head, rest])


def edge_table():
    slot, place = np.arange(half), np.arange(lanes)
    zero = np.zeros((half, lanes))
    phase = [2.0 * np.pi / (8 * lanes) * (np.outer(8 * slot + r, place) % (8 * lanes)) for r in (0, 4)]
    rows = [np.block([[f(phase[0]), zero], [zero, f(phase[1])]]) for f in (np.cos, np.sin)]
    return split_table(np.concatenate([rows[0], -rows[1]]))


def short_tables():
    turns = np.outer(np.arange(lanes), np.arange(lanes)) % lanes
    phase = turns * (2.0 * np.pi / lanes)
    c, s = np.cos(phase), np.sin(phase)
    return split_table(np.block([[c, -s], [s, c]])), split_table(np.block([[c, s], [-s, c]]))


def twiddle_table(radix):
    phase = np.outer(np.arange(radix), np.arange(lanes)) * (2.0 * np.pi / (radix * lanes))
    pair = np.stack([np.cos(phase), np.sin(phase)]).astype(np.float32)
    return np.ascontiguousarray(np.broadcast_to(pair[:, :, None], (2, radix, sublanes, lanes)))


def split(value):
    head = value.astype(jnp.bfloat16)
    return head, (value - head.astype(jnp.float32)).astype(jnp.bfloat16)


def product(left, right, dims):
    dot = functools.partial(
        lax.dot_general, dimension_numbers=(dims, ((), ())), preferred_element_type=jnp.float32
    )
    return dot(left[0], right[0]) + (dot(left[1], right[0]) + dot(left[0], right[1]))


def sine_cosine(angle):
    square = angle * angle
    sine = jnp.full_like(angle, 1.0 / math.factorial(13))
    for order in (11, 9, 7, 5, 3, 1):
        sine = (-1.0) ** ((order - 1) // 2) / math.factorial(order) + square * sine
    cosine = jnp.full_like(angle, -1.0 / math.factorial(14))
    for order in (12, 10, 8, 6, 4, 2, 0):
        cosine = (-1.0) ** (order // 2) / math.factorial(order) + square * cosine
    return angle * sine, cosine


def first_kernel(
    polar_hbm, azimuth_hbm, saturation_hbm, edge_hbm, back_hbm, twiddle_hbm, moment_hbm, side_hbm, out_hbm,
    angle_ref, edge_ref, back_ref, twiddle_ref, moment_ref, side_ref, rows_ref, in_sem, out_sem,
):
    rows, cell_count = angle_ref.shape[1:]
    sources = (polar_hbm, azimuth_hbm, saturation_hbm, edge_hbm, back_hbm, twiddle_hbm)
    places = (angle_ref.at[0], angle_ref.at[1], angle_ref.at[2], edge_ref, back_ref, twiddle_ref)
    loads = [
        pltpu.make_async_copy(source, place, in_sem.at[n])
        for n, (source, place) in enumerate(zip(sources, places))
    ]
    for copy in loads:
        copy.start()
    for copy in loads:
        copy.wait()
    sin_polar, cos_polar = sine_cosine(angle_ref[0])
    sin_half, cos_half = sine_cosine(0.5 * angle_ref[1])
    saturation = angle_ref[2]
    moment = (
        sin_polar * (1.0 - 2.0 * sin_half * sin_half),
        sin_polar * (2.0 * sin_half * cos_half),
        cos_polar,
    )
    groups = [[] for _ in range(4)]
    for c in range(3):
        moment_ref[c] = moment[c]
        side_ref[0, c : c + 1] = moment[c][:1]
        side_ref[1, c : c + 1] = moment[c][rows - 1 :]
        magnet = moment[c] * saturation
        a = [magnet[:, p * lanes : (p + 1) * lanes] for p in range(4)]
        even, odd = a[0] + a[2], a[1] + a[3]
        turned, mixed = root_half * (a[1] - a[3]), root_half * odd
        groups[0].append((even + odd, even - odd))
        for r, (real, imag) in (
            (1, (a[0] + turned, -a[2] - mixed)),
            (2, (a[0] - a[2], a[3] - a[1])),
            (3, (a[0] - turned, a[2] - mixed)),
        ):
            cosine, sine = twiddle_ref[0, r, :1], twiddle_ref[1, r, :1]
            groups[r].append((real * cosine + imag * sine, imag * cosine - real * sine))
    blank = jnp.zeros((rows, 2 * lanes), jnp.bfloat16)
    dims = ((1,), (1,))
    for g in range(4):
        parts = [split(jnp.concatenate(pair, axis=1)) for pair in groups[g]]
        for_real = [jnp.concatenate([part[n] for part in parts] + [blank]) for n in range(2)]
        for_imag = [jnp.concatenate([blank] + [part[n] for part in parts]) for n in range(2)]
        table_ref = edge_ref if g == 0 else back_ref
        real = product((table_ref[0, :lanes], table_ref[1, :lanes]), for_real, dims)
        imag = product((table_ref[0, lanes:], table_ref[1, lanes:]), for_imag, dims)
        cut = slice(g * lanes, (g + 1) * lanes)
        rows_ref[cut, :lanes] = real[:, :lanes]
        rows_ref[cut, lanes : 2 * lanes] = real[:, lanes:] + imag[:, :lanes]
        rows_ref[cut, 2 * lanes :] = imag[:, lanes:]
    sends = [
        pltpu.make_async_copy(rows_ref, out_hbm, out_sem.at[0]),
        pltpu.make_async_copy(moment_ref, moment_hbm, out_sem.at[1]),
        pltpu.make_async_copy(side_ref, side_hbm, out_sem.at[2]),
    ]
    for copy in sends:
        copy.start()
    for copy in sends:
        copy.wait()


def factors(wave_x, wave_y):
    magnitude = jnp.sqrt(wave_x * wave_x + wave_y * wave_y)
    nonzero = magnitude > 0.0
    safe = jnp.where(nonzero, magnitude, 1.0)
    inverse = 1.0 / safe
    series = jnp.ones_like(safe)
    for order in range(9, 1, -1):
        series = 1.0 - series * safe * (1.0 / order)
    growth = jnp.exp(safe)
    lost = jnp.where(safe < 0.5, series * safe, 1.0 - jnp.exp(-safe))
    self_part = jnp.where(nonzero, lost * inverse, 1.0)
    mutual = jnp.where(nonzero, lost * lost * growth * (0.5 * inverse), 0.0)
    decay = jnp.exp(-spacing * magnitude)
    unit_x = jnp.where(nonzero, wave_x * inverse, 0.0)
    unit_y = jnp.where(nonzero, wave_y * inverse, 0.0)
    return unit_x, unit_y, self_part, mutual, decay


def coef_kernel(base_ref, out_ref, *, cell_count):
    pad_length = 2 * cell_count
    radix = pad_length // lanes
    step = math.pi / side_length
    slots = out_ref.shape[2]
    shape = (slots, lanes)
    slot = base_ref[0] * slots + lax.broadcasted_iota(jnp.int32, shape, 0)
    group, order = slot // lanes, slot % lanes
    first = jnp.where(order < half, order * radix, (order - half) * radix + radix // 2)
    wave = jnp.where(group == 0, first, order * radix + group)
    wave_y = step * jnp.where(wave < cell_count, wave, wave - pad_length).astype(jnp.float32)
    weight = jnp.where(wave == 0, 1.0, 2.0) / float(pad_length * pad_length)
    signed = jnp.where(wave % 2 == 0, weight, -weight)
    for r in range(radix):
        index = lax.broadcasted_iota(jnp.int32, shape, 1) * radix + r
        middle = index == cell_count
        folded = jnp.where(index < cell_count, index, index - pad_length)
        wave_x = step * folded.astype(jnp.float32)
        unit_x, unit_y, self_part, mutual, decay = factors(wave_x, wave_y)
        out_ref[0, r] = jnp.where(middle, 0.0, unit_x)
        out_ref[1, r] = unit_y
        out_ref[2, r] = (1.0 - self_part) * weight
        out_ref[3, r] = self_part * weight
        out_ref[4, r] = mutual * weight
        out_ref[5, r] = decay
        edge = jnp.full(shape, -step * cell_count, jnp.float32)
        edge_x, edge_y, self_part, mutual, decay = factors(wave_x, edge)
        rest = (1.0 - self_part) * signed
        mutual = mutual * signed
        square = edge_y * edge_y
        out_ref[6, r] = jnp.where(middle, 0.0, edge_x)
        out_ref[7, r] = rest
        out_ref[8, r] = self_part * signed
        out_ref[9, r] = mutual
        out_ref[10, r] = decay
        out_ref[11, r] = rest * square
        out_ref[12, r] = mutual * square


def neighbours(values, decay):
    count = len(values)
    under = [None] * count
    over = [None] * count
    for t in range(1, count):
        under[t] = decay * (values[t - 1] if under[t - 1] is None else under[t - 1] + values[t - 1])
    for t in range(count - 2, -1, -1):
        over[t] = decay * (values[t + 1] if over[t + 1] is None else over[t + 1] + values[t + 1])
    return under, over


def joined(first, second, sign=1.0):
    if first is None:
        return second if sign > 0.0 else -second
    if second is None:
        return first
    return first + second if sign > 0.0 else first - second


def drive(x, z, keep, mutual, decay, own):
    count = len(x)
    up_r, over_r = [z[t][0] + x[t][1] for t in range(count)], [x[t][1] - z[t][0] for t in range(count)]
    up_i, over_i = [z[t][1] - x[t][0] for t in range(count)], [-z[t][1] - x[t][0] for t in range(count)]
    below_r, below_i = neighbours(up_r, decay)[0], neighbours(up_i, decay)[0]
    above_r, above_i = neighbours(over_r, decay)[1], neighbours(over_i, decay)[1]
    inner, outer = [], []
    for t in range(count):
        total_r, total_i = joined(below_r[t], above_r[t]), joined(below_i[t], above_i[t])
        differ_r = joined(below_r[t], above_r[t], -1.0)
        differ_i = joined(below_i[t], above_i[t], -1.0)
        inner.append((mutual * total_i - keep * x[t][0], -(mutual * total_r) - keep * x[t][1]))
        outer.append((mutual * differ_r - own * z[t][0], mutual * differ_i - own * z[t][1]))
    return inner, outer


def even_part(values, keep, mutual, decay):
    out = []
    for n in range(2):
        part = [v[n] for v in values]
        under, over = neighbours(part, decay)
        out.append([-(keep * part[t]) - mutual * joined(under[t], over[t]) for t in range(len(part))])
    return list(zip(*out))


def respond(spectrum, coef, has_middle, middle):
    count = len(spectrum)
    unit_x, unit_y, keep, own, mutual, decay = coef[:6]
    edge_x, edge_keep, edge_own, edge_mutual, edge_decay, keep_y, mutual_y = coef[6:]
    x = [s[0] for s in spectrum]
    y = [s[1] for s in spectrum]
    z = [s[2] for s in spectrum]
    charge = [tuple(unit_x * x[t][n] + unit_y * y[t][n] for n in range(2)) for t in range(count)]
    inner, outer = drive(charge, z, keep, mutual, decay, own)
    charge = [tuple(edge_x * x[t][n] for n in range(2)) for t in range(count)]
    edge_inner, edge_outer = drive(charge, z, edge_keep, edge_mutual, edge_decay, edge_own)
    edge_y = even_part(y, keep_y, mutual_y, edge_decay)
    out = []
    for t in range(count):
        out.append(
            [
                tuple(unit_x * inner[t][n] - edge_x * edge_inner[t][n] for n in range(2)),
                tuple(unit_y * inner[t][n] - edge_y[t][n] for n in range(2)),
                tuple(outer[t][n] - edge_outer[t][n] for n in range(2)),
            ]
        )
    if has_middle:
        square = jnp.where(middle, 1.0 - unit_y * unit_y, 0.0)
        alone = even_part(x, keep * square, mutual * square, decay)
        keep_m, mutual_m = jnp.where(middle, keep_y, 0.0), jnp.where(middle, mutual_y, 0.0)
        cross_x = even_part(x, keep_m, mutual_m, edge_decay)
        cross_y = even_part(y, keep_m, mutual_m, edge_decay)
        for t in range(count):
            out[t][0] = tuple(
                out[t][0][n] + alone[t][n] - cross_x[t][n] - cross_y[t][n] for n in range(2)
            )
            out[t][1] = tuple(out[t][1][n] - cross_x[t][n] for n in range(2))
    return out


def add(a, b):
    return a[0] + b[0], a[1] + b[1]


def sub(a, b):
    return a[0] - b[0], a[1] - b[1]


def add_turned(a, b):
    return a[0] - b[1], a[1] + b[0]


def sub_turned(a, b):
    return a[0] + b[1], a[1] - b[0]


def four_point(z):
    s, d, u, v = add(z[0], z[2]), sub(z[0], z[2]), add(z[1], z[3]), sub(z[1], z[3])
    return add(s, u), sub_turned(d, v), sub(s, u), add_turned(d, v)


def four_point_back(z):
    s, d, u, v = add(z[0], z[2]), sub(z[0], z[2]), add(z[1], z[3]), sub(z[1], z[3])
    return add(s, u), add_turned(d, v), sub(s, u), sub_turned(d, v)


def spread(z):
    turned = [
        z[0],
        (root_half * (z[1][0] + z[1][1]), root_half * (z[1][1] - z[1][0])),
        (z[2][1], -z[2][0]),
        (root_half * (z[3][1] - z[3][0]), -root_half * (z[3][0] + z[3][1])),
    ]
    even, odd = four_point(z), four_point(turned)
    return [even[r // 2] if r % 2 == 0 else odd[r // 2] for r in range(8)]


def gather_back(v):
    even, odd = four_point_back(v[0::2]), four_point_back(v[1::2])
    return [
        add(even[0], odd[0]),
        (even[1][0] + root_half * (odd[1][0] - odd[1][1]), even[1][1] + root_half * (odd[1][0] + odd[1][1])),
        add_turned(even[2], odd[2]),
        (even[3][0] - root_half * (odd[3][0] + odd[3][1]), even[3][1] + root_half * (odd[3][0] - odd[3][1])),
    ]


def middle_kernel(rows_ref, coef_ref, twiddle_ref, forward_ref, back_ref, out_ref, work_ref, *, layers):
    radix = twiddle_ref.shape[1]
    pieces = radix // 2
    items = layers * 3
    place = lax.broadcasted_iota(jnp.int32, (sublanes, lanes), 1)
    low = place < half
    dims = ((1,), (0,))
    forward = (forward_ref[0], forward_ref[1])
    back = (back_ref[0], back_ref[1])

    def piece(plane, layer, part):
        tile, upper = divmod(part, 2)
        cut = slice(tile * lanes, (tile + 1) * lanes)
        row = plane * layers + layer
        first, second = rows_ref[row, :, cut], rows_ref[row + layers, :, cut]
        if upper:
            return jnp.where(low, pltpu.roll(first, half, 1), second)
        return jnp.where(low, first, pltpu.roll(second, half, 1))

    for item in range(items):
        layer, c = divmod(item, 3)
        z = [(piece(2 * p, layer, c), piece(2 * p, layer, 3 + c)) for p in range(pieces)]
        for r, (real, imag) in enumerate(spread(z)):
            if r > 0:
                cosine, sine = twiddle_ref[0, r], twiddle_ref[1, r]
                real, imag = real * cosine + imag * sine, imag * cosine - real * sine
            start = item * sublanes
            work_ref[r, start : start + sublanes, :lanes] = real
            work_ref[r, start : start + sublanes, lanes:] = imag
    for r in range(radix):
        value = product(split(work_ref[r]), forward, dims)
        spectrum = [
            [
                (
                    value[(t * 3 + c) * sublanes : (t * 3 + c + 1) * sublanes, :lanes],
                    value[(t * 3 + c) * sublanes : (t * 3 + c + 1) * sublanes, lanes:],
                )
                for c in range(3)
            ]
            for t in range(layers)
        ]
        coef = [coef_ref[n, r] for n in range(coef_count)]
        out = respond(spectrum, coef, r == 0, place * radix + r == radix * half)
        value = jnp.concatenate(
            [jnp.concatenate([pair[0], pair[1]], axis=1) for layer in out for pair in layer]
        )
        work_ref[r] = product(split(value), back, dims)
    for layer in range(layers):
        parts = [[None] * 6 for _ in range(pieces)]
        for c in range(3):
            start = (layer * 3 + c) * sublanes
            v = []
            for r in range(radix):
                real = work_ref[r, start : start + sublanes, :lanes]
                imag = work_ref[r, start : start + sublanes, lanes:]
                if r > 0:
                    cosine, sine = twiddle_ref[0, r], twiddle_ref[1, r]
                    real, imag = real * cosine - imag * sine, imag * cosine + real * sine
                v.append((real, imag))
            for p, (real, imag) in enumerate(gather_back(v)):
                parts[p][c], parts[p][3 + c] = real, imag
        for p in range(pieces):
            for tile in range(3):
                first, second = parts[p][2 * tile], parts[p][2 * tile + 1]
                cut = slice(tile * lanes, (tile + 1) * lanes)
                row = 2 * p * layers + layer
                out_ref[row, :, cut] = jnp.where(low, first, pltpu.roll(second, half, 1))
                out_ref[row + layers, :, cut] = jnp.where(low, pltpu.roll(first, half, 1), second)


def exchange_kernel(link_ref, moment_ref, below_ref, above_ref, before_ref, after_ref, anisotropy_ref, out_ref):
    rows, cell_count = anisotropy_ref.shape
    row = lax.broadcasted_iota(jnp.int32, (rows, cell_count), 0)
    column = lax.broadcasted_iota(jnp.int32, (rows, cell_count), 1)
    stiffness, lower_link, upper_link = link_ref[0], link_ref[1], link_ref[2]
    for c in range(3):
        m = moment_ref[c]
        before = jnp.where(row == 0, before_ref[c : c + 1], pltpu.roll(m, 1, 0))
        after = jnp.where(row == rows - 1, after_ref[c : c + 1], pltpu.roll(m, rows - 1, 0))
        left = jnp.where(column == 0, 0.0, pltpu.roll(m, 1, 1))
        right = jnp.where(column == cell_count - 1, 0.0, pltpu.roll(m, cell_count - 1, 1))
        total = stiffness * (before + after + left + right)
        total = total + lower_link * below_ref[c] + upper_link * above_ref[c]
        if c == 2:
            total = total + anisotropy_ref[...] * m
        out_ref[c] = total


def last_kernel(
    moment_ref, other_ref, edge_ref, back_ref, twiddle_ref, block_ref, field_ref, out_ref
):
    rows = moment_ref.shape[1]
    turned = block_ref[...].T
    dims = ((1,), (0,))
    waves = []
    for g in range(4):
        cut = slice(g * lanes, (g + 1) * lanes)
        value = jnp.concatenate([turned[: 3 * rows, cut], turned[3 * rows :, cut]], axis=1)
        table_ref = edge_ref if g == 0 else back_ref
        value = product(split(value), (table_ref[0], table_ref[1]), dims)
        real, imag = value[:, :lanes], value[:, lanes:]
        if g > 0:
            cosine, sine = twiddle_ref[0, g, :1], twiddle_ref[1, g, :1]
            real, imag = real * cosine - imag * sine, imag * cosine + real * sine
        waves.append((real, imag))
    even, odd = waves[0][0] + waves[0][1], waves[0][0] - waves[0][1]
    (real_1, imag_1), (real_2, imag_2), (real_3, imag_3) = waves[1:]
    flat, tilted = root_half * (real_1 - real_3), root_half * (imag_1 + imag_3)
    demag = jnp.concatenate(
        [
            even + real_1 + real_2 + real_3,
            odd + flat - tilted - imag_2,
            even - imag_1 - real_2 + imag_3,
            odd - flat - tilted + imag_2,
        ],
        axis=1,
    )
    span = rows // piece_count
    for n in range(piece_count):
        cut = pl.ds(n * span, span)
        m = [moment_ref[c, cut] for c in range(3)]
        f = [other_ref[c, cut] + demag[c * rows + n * span : c * rows + (n + 1) * span] for c in range(3)]
        for c in range(3):
            field_ref[c, cut] = f[c]
        first = cross(m, f)
        second = cross(m, first)
        stepped = []
        for c in range(3):
            torque = -(first[c] + damping * second[c]) / (1.0 + damping * damping)
            stepped.append(m[c] + time_step * torque)
        scale = lax.rsqrt(stepped[0] * stepped[0] + stepped[1] * stepped[1] + stepped[2] * stepped[2])
        for c in range(3):
            out_ref[c, cut] = stepped[c] * scale


def cross(first, second):
    return [
        first[1] * second[2] - first[2] * second[1],
        first[2] * second[0] - first[0] * second[2],
        first[0] * second[1] - first[1] * second[0],
    ]


def shift(value, axis, step):
    count = lax.axis_size(axis)
    pairs = [(i, i + step) for i in range(count) if 0 <= i + step < count]
    return lax.ppermute(value, axis, pairs)


def fast_body(polar, azimuth, saturation, anisotropy, stiffness, coupling):
    rows, cell_count = polar.shape[1:]
    layers, planes = lax.axis_size("layer"), lax.axis_size("plane")
    device_count = layers * planes
    layer_index = lax.axis_index("layer")
    plane_index = lax.axis_index("plane")
    slots = cell_count // device_count
    radix = 2 * cell_count // lanes
    width = 6 * rows
    f32, bf16 = jnp.float32, jnp.bfloat16
    edge = jnp.asarray(edge_table())
    forward, back = (jnp.asarray(t) for t in short_tables())
    twiddle = jnp.asarray(twiddle_table(radix))
    field_shape = jax.ShapeDtypeStruct((3, rows, cell_count), f32)
    side_shape = (2, sublanes, cell_count)
    block_shape = jax.ShapeDtypeStruct((cell_count, width), f32)
    small = pltpu.CompilerParams(vmem_limit_bytes=vmem_limit)
    dma = pltpu.SemaphoreType.DMA
    flops = 12 * rows * cell_count * cell_count * 6

    moment, side, block = pl.pallas_call(
        first_kernel,
        out_shape=[field_shape, jax.ShapeDtypeStruct(side_shape, f32), block_shape],
        in_specs=[in_any] * 6,
        out_specs=[in_any] * 3,
        scratch_shapes=[
            pltpu.VMEM((3, rows, cell_count), f32),
            pltpu.VMEM(edge.shape, bf16),
            pltpu.VMEM(back.shape, bf16),
            pltpu.VMEM(twiddle.shape, f32),
            pltpu.VMEM((3, rows, cell_count), f32),
            pltpu.VMEM(side_shape, f32),
            pltpu.VMEM((cell_count, width), f32),
            dma((6,)),
            dma((3,)),
        ],
        cost_estimate=pl.CostEstimate(flops=flops, bytes_accessed=4 << 20, transcendentals=0),
        name="first",
    )(polar[0], azimuth[0], saturation[0], edge, back, twiddle)

    base = (plane_index * layers + layer_index).astype(jnp.int32).reshape(1)
    coefs = pl.pallas_call(
        functools.partial(coef_kernel, cell_count=cell_count),
        out_shape=jax.ShapeDtypeStruct((coef_count, radix, slots, lanes), f32),
        in_specs=[in_smem],
        out_specs=in_vmem,
        compiler_params=small,
        cost_estimate=pl.CostEstimate(flops=20 << 20, bytes_accessed=1 << 20, transcendentals=1 << 16),
        name="coefs",
    )(base)

    below = shift(moment, "layer", 1)
    above = shift(moment, "layer", -1)
    before = shift(side[1], "plane", 1)
    after = shift(side[0], "plane", -1)
    links = jnp.stack(
        [
            stiffness[0],
            coupling[jnp.maximum(layer_index - 1, 0)],
            coupling[jnp.minimum(layer_index, coupling.shape[0] - 1)],
        ]
    )
    other = pl.pallas_call(
        exchange_kernel,
        out_shape=field_shape,
        in_specs=[in_smem] + [in_vmem] * 6,
        out_specs=in_vmem,
        compiler_params=small,
        cost_estimate=pl.CostEstimate(flops=20 << 20, bytes_accessed=2 << 20, transcendentals=0),
        name="exchange",
    )(links, moment, below, above, before, after, anisotropy[0])

    exchange_all = functools.partial(
        lax.all_to_all, axis_name=both, split_axis=0, concat_axis=0, tiled=True
    )
    block = exchange_all(block.reshape(device_count, slots, width))
    block = pl.pallas_call(
        functools.partial(middle_kernel, layers=layers),
        out_shape=jax.ShapeDtypeStruct((device_count, slots, width), f32),
        grid=(slots // sublanes,),
        in_specs=[
            pl.BlockSpec((device_count, sublanes, width), lambda g: (0, g, 0)),
            pl.BlockSpec((coef_count, radix, sublanes, lanes), lambda g: (0, 0, g, 0)),
            pl.BlockSpec(twiddle.shape, lambda g: (0, 0, 0, 0)),
            pl.BlockSpec(forward.shape, lambda g: (0, 0, 0)),
            pl.BlockSpec(back.shape, lambda g: (0, 0, 0)),
        ],
        out_specs=pl.BlockSpec((device_count, sublanes, width), lambda g: (0, g, 0)),
        scratch_shapes=[pltpu.VMEM((radix, layers * 3 * sublanes, 2 * lanes), f32)],
        compiler_params=small,
        cost_estimate=pl.CostEstimate(flops=2000 << 20, bytes_accessed=4 << 20, transcendentals=0),
        name="middle",
    )(block, coefs, twiddle, forward, back)
    block = exchange_all(block)

    field, stepped = pl.pallas_call(
        last_kernel,
        out_shape=[field_shape] * 2,
        in_specs=[in_vmem] * 6,
        out_specs=[in_vmem] * 2,
        compiler_params=small,
        cost_estimate=pl.CostEstimate(flops=flops, bytes_accessed=4 << 20, transcendentals=0),
        name="last",
    )(moment, other, edge, back, twiddle, block.reshape(cell_count, width))
    return field[None], stepped[None]


def with_halo(cells, sides, width):
    for axis, dim in sides:
        count = lax.axis_size(axis)
        ends = count - 1
        head = lax.slice_in_dim(cells, 0, width, axis=dim)
        tail = lax.slice_in_dim(cells, cells.shape[dim] - width, cells.shape[dim], axis=dim)
        cells = jnp.concatenate(
            [
                lax.ppermute(tail, axis, [(i, (i + 1) % count) for i in range(ends)]),
                cells,
                lax.ppermute(head, axis, [((i + 1) % count, i) for i in range(ends)]),
            ],
            axis=dim,
        )
    return cells


def cross_product(first, second):
    return jnp.stack(
        [
            first[1] * second[2] - first[2] * second[1],
            first[2] * second[0] - first[0] * second[2],
            first[0] * second[1] - first[1] * second[0],
        ]
    )


def signed_wave(index, cell_count):
    folded = jnp.where(index < cell_count, index, index - 2 * cell_count)
    return jnp.pi * folded.astype(jnp.float32) / side_length


def plain_body(polar, azimuth, saturation, anisotropy, stiffness, coupling):
    row_count = polar.shape[1]
    cell_count = polar.shape[2]
    pad_length = 2 * cell_count
    plane_count = lax.axis_size("plane")
    band_width = pad_length // plane_count
    layer_index = lax.axis_index("layer")
    plane_index = lax.axis_index("plane")
    theta = polar[0]
    azimuthal = azimuth[0]
    moment_in = jnp.stack(
        [jnp.sin(theta) * jnp.cos(azimuthal), jnp.sin(theta) * jnp.sin(azimuthal), jnp.cos(theta)]
    )
    magnet = moment_in * saturation[0][None]
    place = jnp.arange(cell_count, dtype=jnp.int32)
    wave_index = jnp.arange(pad_length, dtype=jnp.int32)
    turns = place[:, None] * wave_index[None, :] % pad_length
    phase = turns.astype(jnp.float32) * (2.0 * jnp.pi / pad_length)
    cosine = jnp.cos(phase)
    sine = jnp.sin(phase)
    cosine_blocks = cosine.reshape(plane_count, row_count, pad_length)
    sine_blocks = sine.reshape(plane_count, row_count, pad_length)
    cosine_bands = cosine.reshape(cell_count, plane_count, band_width)
    sine_bands = sine.reshape(cell_count, plane_count, band_width)
    along_real = jnp.einsum("cxy,yk->ckx", magnet, cosine, precision=exact)
    along_imag = -jnp.einsum("cxy,yk->ckx", magnet, sine, precision=exact)
    sectioned = jnp.stack([along_real, along_imag], 1).reshape(
        3, 2, plane_count, band_width * row_count
    )
    block = lax.all_to_all(sectioned, "plane", split_axis=2, concat_axis=2, tiled=True)
    item_count = block.shape[0]
    split = block.reshape(item_count, 2, plane_count, band_width, row_count)
    with_cosine = jnp.einsum("npsqx,sxk->npqk", split, cosine_blocks, precision=exact)
    with_sine = jnp.einsum("npsqx,sxk->npqk", split, sine_blocks, precision=exact)
    spectrum = jnp.stack(
        [with_cosine[:, 0] + with_sine[:, 1], with_cosine[:, 1] - with_sine[:, 0]], 1
    )
    wave_y = signed_wave(
        plane_index * band_width + jnp.arange(band_width, dtype=jnp.int32), cell_count
    )[:, None]
    wave_x = signed_wave(wave_index, cell_count)[None, :]
    magnitude = jnp.sqrt(wave_x * wave_x + wave_y * wave_y)
    nonzero = magnitude > 0.0
    safe = jnp.where(nonzero, magnitude, 1.0)
    unit_x = jnp.where(nonzero, wave_x / safe, 0.0)
    unit_y = jnp.where(nonzero, wave_y / safe, 0.0)
    self_part = jnp.where(nonzero, -jnp.expm1(-safe) / safe, 1.0)
    half_sinh = jnp.sinh(0.5 * safe)
    mutual = jnp.where(nonzero, 2.0 * half_sinh * half_sinh / safe, 0.0)
    spectral_x = spectrum[0]
    spectral_y = spectrum[1]
    spectral_z = spectrum[2]
    inplane = unit_x * spectral_x + unit_y * spectral_y
    upward = jnp.stack([spectral_z[0] + inplane[1], spectral_z[1] - inplane[0]])
    downward = jnp.stack([-spectral_z[0] + inplane[1], -spectral_z[1] - inplane[0]])
    emitted = jnp.stack([upward, downward])[None]
    piece = lax.all_gather(emitted, "layer", axis=0, tiled=True)
    source = jnp.arange(piece.shape[0], dtype=jnp.int32)
    separation = layer_index - source
    distance = jnp.abs(separation).astype(jnp.float32)
    weight = jnp.exp(-spacing * distance[:, None, None] * magnitude[None])
    lower = jnp.where((separation > 0)[:, None, None], weight, 0.0)
    upper = jnp.where((separation < 0)[:, None, None], weight, 0.0)
    below = jnp.sum(lower[:, None] * piece[:, 0], 0)
    above = jnp.sum(upper[:, None] * piece[:, 1], 0)
    total = below + above
    differ = below - above
    remainder = 1.0 - self_part
    field_x = jnp.stack(
        [
            -remainder * unit_x * inplane[0] + unit_x * mutual * total[1],
            -remainder * unit_x * inplane[1] - unit_x * mutual * total[0],
        ]
    )
    field_y = jnp.stack(
        [
            -remainder * unit_y * inplane[0] + unit_y * mutual * total[1],
            -remainder * unit_y * inplane[1] - unit_y * mutual * total[0],
        ]
    )
    field_z = jnp.stack(
        [
            -self_part * spectral_z[0] + mutual * differ[0],
            -self_part * spectral_z[1] + mutual * differ[1],
        ]
    )
    spectral = jnp.stack([field_x, field_y, field_z])
    back_cosine = jnp.einsum("cpqk,sxk->cpsqx", spectral, cosine_blocks, precision=exact)
    back_sine = jnp.einsum("cpqk,sxk->cpsqx", spectral, sine_blocks, precision=exact)
    returned = jnp.stack(
        [back_cosine[:, 0] - back_sine[:, 1], back_sine[:, 0] + back_cosine[:, 1]], 1
    )
    returned = returned.reshape(3, 2, plane_count, band_width * row_count)
    scale = 1.0 / (float(pad_length) * float(pad_length))
    block = lax.all_to_all(returned, "plane", split_axis=2, concat_axis=2, tiled=True)
    item_count = block.shape[0]
    split = block.reshape(item_count, 2, plane_count, band_width, row_count)
    real_part = jnp.einsum("nsqx,ysq->nxy", split[:, 0], cosine_bands, precision=exact)
    imag_part = jnp.einsum("nsqx,ysq->nxy", split[:, 1], sine_bands, precision=exact)
    demag = (real_part - imag_part) * scale
    padded = with_halo(moment_in[None], (("layer", 0), ("plane", 2)), 1)
    centre = padded[1]
    beside = centre[:, :-2] + centre[:, 2:]
    sideways = jnp.pad(moment_in, ((0, 0), (0, 0), (1, 1)))
    beside = beside + sideways[:, :, :-2] + sideways[:, :, 2:]
    lower_link = coupling[jnp.maximum(layer_index - 1, 0)]
    upper_link = coupling[jnp.minimum(layer_index, coupling.shape[0] - 1)]
    exchange_field = (
        stiffness[0] * beside + lower_link * padded[0, :, 1:-1] + upper_link * padded[2, :, 1:-1]
    )
    flat_zero = jnp.zeros_like(moment_in[2])
    uniaxial = jnp.stack([flat_zero, flat_zero, anisotropy[0] * moment_in[2]])
    field = demag + exchange_field + uniaxial
    first_cross = cross_product(moment_in, field)
    second_cross = cross_product(moment_in, first_cross)
    torque = -(first_cross + damping * second_cross) / (1.0 + damping * damping)
    stepped = moment_in + time_step * torque
    length = jnp.sqrt(jnp.sum(stepped * stepped, axis=0, keepdims=True))
    return (field[None], (stepped / length)[None])


def body(polar, azimuth, saturation, anisotropy, stiffness, coupling):
    rows, cell_count = polar.shape[1:]
    device_count = lax.axis_size("layer") * lax.axis_size("plane")
    fits = 2 * rows == lanes and cell_count == 4 * lanes
    fits = fits and cell_count % (device_count * sublanes) == 0
    chosen = fast_body if fits else plain_body
    return chosen(polar, azimuth, saturation, anisotropy, stiffness, coupling)


def solution(mesh):
    placed = (
        P("layer", "plane", None),
        P("layer", "plane", None),
        P("layer", "plane", None),
        P("layer", "plane", None),
        P("layer"),
        P(),
    )
    return jax.shard_map(
        body,
        mesh=mesh,
        in_specs=placed,
        out_specs=(P("layer", None, "plane", None), P("layer", None, "plane", None)),
        check_vma=False,
    )
```

```python
import functools
import math

import jax
import jax.numpy as jnp
import numpy as np
from jax import lax
from jax.experimental import pallas as pl
from jax.experimental.pallas import tpu as pltpu
from jax.sharding import PartitionSpec as P

side_length = 512.0
spacing = 1.2
damping = 0.1
time_step = 0.1
exact = lax.Precision.HIGHEST

lanes = 128
sublanes = 8
half = lanes // 2
root_half = math.sqrt(0.5)
piece_count = 2
coef_count = 6
vmem_limit = 16 << 20
both = ("plane", "layer")
in_vmem = pl.BlockSpec(memory_space=pltpu.VMEM)
in_any = pl.BlockSpec(memory_space=pl.ANY)
in_smem = pl.BlockSpec(memory_space=pltpu.SMEM)


def split_table(table):
    head = table.astype(np.float32).astype(jnp.bfloat16)
    rest = (table - head.astype(np.float64)).astype(np.float32).astype(jnp.bfloat16)
    return np.stack([head, rest])


def edge_table():
    slot, place = np.arange(half), np.arange(lanes)
    zero = np.zeros((half, lanes))
    phase = [2.0 * np.pi / (8 * lanes) * (np.outer(8 * slot + r, place) % (8 * lanes)) for r in (0, 4)]
    rows = [np.block([[f(phase[0]), zero], [zero, f(phase[1])]]) for f in (np.cos, np.sin)]
    return split_table(np.concatenate([rows[0], -rows[1]]))


def short_tables():
    turns = np.outer(np.arange(lanes), np.arange(lanes)) % lanes
    phase = turns * (2.0 * np.pi / lanes)
    c, s = np.cos(phase), np.sin(phase)
    return split_table(np.block([[c, -s], [s, c]])), split_table(np.block([[c, s], [-s, c]]))


def twiddle_table(radix):
    phase = np.outer(np.arange(radix), np.arange(lanes)) * (2.0 * np.pi / (radix * lanes))
    pair = np.stack([np.cos(phase), np.sin(phase)]).astype(np.float32)
    return np.ascontiguousarray(np.broadcast_to(pair[:, :, None], (2, radix, sublanes, lanes)))


def split(value):
    head = value.astype(jnp.bfloat16)
    return head, (value - head.astype(jnp.float32)).astype(jnp.bfloat16)


def product(left, right, dims):
    (axis,), (other,) = dims
    return lax.dot_general(
        jnp.concatenate([left[0], left[1], left[0]], axis=axis),
        jnp.concatenate([right[0], right[0], right[1]], axis=other),
        dimension_numbers=(dims, ((), ())),
        preferred_element_type=jnp.float32,
    )


def sine_cosine(angle):
    square = angle * angle
    sine = jnp.full_like(angle, 1.0 / math.factorial(13))
    for order in (11, 9, 7, 5, 3, 1):
        sine = (-1.0) ** ((order - 1) // 2) / math.factorial(order) + square * sine
    cosine = jnp.full_like(angle, -1.0 / math.factorial(14))
    for order in (12, 10, 8, 6, 4, 2, 0):
        cosine = (-1.0) ** (order // 2) / math.factorial(order) + square * cosine
    return angle * sine, cosine


def first_kernel(
    polar_hbm, azimuth_hbm, saturation_hbm, edge_hbm, back_hbm, twiddle_hbm, moment_hbm, side_hbm, out_hbm,
    angle_ref, edge_ref, back_ref, twiddle_ref, moment_ref, side_ref, rows_ref, in_sem, out_sem,
):
    rows, cell_count = angle_ref.shape[1:]
    sources = (polar_hbm, azimuth_hbm, saturation_hbm, edge_hbm, back_hbm, twiddle_hbm)
    places = (angle_ref.at[0], angle_ref.at[1], angle_ref.at[2], edge_ref, back_ref, twiddle_ref)
    loads = [
        pltpu.make_async_copy(source, place, in_sem.at[n])
        for n, (source, place) in enumerate(zip(sources, places))
    ]
    for copy in loads:
        copy.start()
    for copy in loads:
        copy.wait()
    sin_polar, cos_polar = sine_cosine(angle_ref[0])
    sin_half, cos_half = sine_cosine(0.5 * angle_ref[1])
    saturation = angle_ref[2]
    moment = (
        sin_polar * (1.0 - 2.0 * sin_half * sin_half),
        sin_polar * (2.0 * sin_half * cos_half),
        cos_polar,
    )
    groups = [[] for _ in range(4)]
    for c in range(3):
        moment_ref[c] = moment[c]
        side_ref[0, c : c + 1] = moment[c][:1]
        side_ref[1, c : c + 1] = moment[c][rows - 1 :]
        magnet = moment[c] * saturation
        a = [magnet[:, p * lanes : (p + 1) * lanes] for p in range(4)]
        even, odd = a[0] + a[2], a[1] + a[3]
        turned, mixed = root_half * (a[1] - a[3]), root_half * odd
        groups[0].append((even + odd, even - odd))
        for r, (real, imag) in (
            (1, (a[0] + turned, -a[2] - mixed)),
            (2, (a[0] - a[2], a[3] - a[1])),
            (3, (a[0] - turned, a[2] - mixed)),
        ):
            cosine, sine = twiddle_ref[0, r, :1], twiddle_ref[1, r, :1]
            groups[r].append((real * cosine + imag * sine, imag * cosine - real * sine))
    sends = [
        pltpu.make_async_copy(moment_ref, moment_hbm, out_sem.at[0]),
        pltpu.make_async_copy(side_ref, side_hbm, out_sem.at[1]),
    ]
    for copy in sends:
        copy.start()
    blank = jnp.zeros((rows, 2 * lanes), jnp.bfloat16)
    dims = ((1,), (1,))
    for g in range(4):
        parts = [split(jnp.concatenate(pair, axis=1)) for pair in groups[g]]
        for_real = [jnp.concatenate([part[n] for part in parts] + [blank]) for n in range(2)]
        for_imag = [jnp.concatenate([blank] + [part[n] for part in parts]) for n in range(2)]
        table_ref = edge_ref if g == 0 else back_ref
        real = product((table_ref[0, :lanes], table_ref[1, :lanes]), for_real, dims)
        imag = product((table_ref[0, lanes:], table_ref[1, lanes:]), for_imag, dims)
        cut = slice(g * lanes, (g + 1) * lanes)
        rows_ref[cut, :lanes] = real[:, :lanes]
        rows_ref[cut, lanes : 2 * lanes] = real[:, lanes:] + imag[:, :lanes]
        rows_ref[cut, 2 * lanes :] = imag[:, lanes:]
        sends.append(pltpu.make_async_copy(rows_ref.at[cut], out_hbm.at[cut], out_sem.at[2 + g]))
        sends[-1].start()
    for copy in sends:
        copy.wait()


def factors(wave_x, wave_y):
    magnitude = jnp.sqrt(wave_x * wave_x + wave_y * wave_y)
    nonzero = magnitude > 0.0
    safe = jnp.where(nonzero, magnitude, 1.0)
    inverse = 1.0 / safe
    series = jnp.ones_like(safe)
    for order in range(9, 1, -1):
        series = 1.0 - series * safe * (1.0 / order)
    growth = jnp.exp(safe)
    lost = jnp.where(safe < 0.5, series * safe, 1.0 - jnp.exp(-safe))
    self_part = jnp.where(nonzero, lost * inverse, 1.0)
    mutual = jnp.where(nonzero, lost * lost * growth * (0.5 * inverse), 0.0)
    decay = jnp.exp(-spacing * magnitude)
    unit_x = jnp.where(nonzero, wave_x * inverse, 0.0)
    unit_y = jnp.where(nonzero, wave_y * inverse, 0.0)
    return unit_x, unit_y, self_part, mutual, decay


def coef_kernel(base_ref, *refs, cell_count):
    count = len(refs) // 2 - 1
    out_ref, edge_ref, sign_ref = refs[count : count + 3]
    for table_ref, kept_ref in zip(refs[:count], refs[count + 3 :]):
        kept_ref[...] = table_ref[...]
    pad_length = 2 * cell_count
    radix = pad_length // lanes
    step = math.pi / side_length
    slots = out_ref.shape[2]
    shape = (slots, lanes)
    slot = base_ref[0] * slots + lax.broadcasted_iota(jnp.int32, shape, 0)
    group, order = slot // lanes, slot % lanes
    first = jnp.where(order < half, order * radix, (order - half) * radix + radix // 2)
    wave = jnp.where(group == 0, first, order * radix + group)
    wave_y = step * jnp.where(wave < cell_count, wave, wave - pad_length).astype(jnp.float32)
    weight = jnp.where(wave == 0, 1.0, 2.0) / float(pad_length * pad_length)
    sign_ref[...] = jnp.where(wave % 2 == 0, weight, -weight)
    for r in range(radix):
        index = lax.broadcasted_iota(jnp.int32, shape, 1) * radix + r
        folded = jnp.where(index < cell_count, index, index - pad_length)
        unit_x, unit_y, self_part, mutual, decay = factors(step * folded.astype(jnp.float32), wave_y)
        out_ref[0, r] = jnp.where(index == cell_count, 0.0, unit_x)
        out_ref[1, r] = unit_y
        out_ref[2, r] = (1.0 - self_part) * weight
        out_ref[3, r] = self_part * weight
        out_ref[4, r] = mutual * weight
        out_ref[5, r] = decay
    shape = (radix, lanes)
    index = lax.broadcasted_iota(jnp.int32, shape, 1) * radix + lax.broadcasted_iota(jnp.int32, shape, 0)
    folded = jnp.where(index < cell_count, index, index - pad_length)
    wave_y = jnp.full(shape, -step * cell_count, jnp.float32)
    edge_x, edge_y, self_part, mutual, decay = factors(step * folded.astype(jnp.float32), wave_y)
    edge_ref[0] = jnp.where(index == cell_count, 0.0, edge_x)
    edge_ref[1] = 1.0 - self_part
    edge_ref[2] = self_part
    edge_ref[3] = mutual
    edge_ref[4] = decay
    edge_ref[5] = edge_y * edge_y


def neighbours(values, decay):
    count = len(values)
    under = [None] * count
    over = [None] * count
    for t in range(1, count):
        under[t] = decay * (values[t - 1] if under[t - 1] is None else under[t - 1] + values[t - 1])
    for t in range(count - 2, -1, -1):
        over[t] = decay * (values[t + 1] if over[t + 1] is None else over[t + 1] + values[t + 1])
    return under, over


def joined(first, second, sign=1.0):
    if first is None:
        return second if sign > 0.0 else -second
    if second is None:
        return first
    return first + second if sign > 0.0 else first - second


def drive(x, z, keep, mutual, decay, own):
    count = len(x)
    up_r, over_r = [z[t][0] + x[t][1] for t in range(count)], [x[t][1] - z[t][0] for t in range(count)]
    up_i, over_i = [z[t][1] - x[t][0] for t in range(count)], [-z[t][1] - x[t][0] for t in range(count)]
    below_r, below_i = neighbours(up_r, decay)[0], neighbours(up_i, decay)[0]
    above_r, above_i = neighbours(over_r, decay)[1], neighbours(over_i, decay)[1]
    inner, outer = [], []
    for t in range(count):
        total_r, total_i = joined(below_r[t], above_r[t]), joined(below_i[t], above_i[t])
        differ_r = joined(below_r[t], above_r[t], -1.0)
        differ_i = joined(below_i[t], above_i[t], -1.0)
        inner.append((mutual * total_i - keep * x[t][0], -(mutual * total_r) - keep * x[t][1]))
        outer.append((mutual * differ_r - own * z[t][0], mutual * differ_i - own * z[t][1]))
    return inner, outer


def even_part(values, keep, mutual, decay):
    out = []
    for n in range(2):
        part = [v[n] for v in values]
        under, over = neighbours(part, decay)
        out.append([-(keep * part[t]) - mutual * joined(under[t], over[t]) for t in range(len(part))])
    return list(zip(*out))


def respond(spectrum, coef, has_middle, middle):
    count = len(spectrum)
    unit_x, unit_y, keep, own, mutual, decay = coef[:6]
    edge_x, edge_keep, edge_own, edge_mutual, edge_decay, square_y, sign = coef[6:]
    edge_keep, edge_own, edge_mutual = sign * edge_keep, sign * edge_own, sign * edge_mutual
    keep_y, mutual_y = square_y * edge_keep, square_y * edge_mutual
    x = [s[0] for s in spectrum]
    y = [s[1] for s in spectrum]
    z = [s[2] for s in spectrum]
    charge = [tuple(unit_x * x[t][n] + unit_y * y[t][n] for n in range(2)) for t in range(count)]
    inner, outer = drive(charge, z, keep, mutual, decay, own)
    charge = [tuple(edge_x * x[t][n] for n in range(2)) for t in range(count)]
    edge_inner, edge_outer = drive(charge, z, edge_keep, edge_mutual, edge_decay, edge_own)
    edge_y = even_part(y, keep_y, mutual_y, edge_decay)
    out = []
    for t in range(count):
        out.append(
            [
                tuple(unit_x * inner[t][n] - edge_x * edge_inner[t][n] for n in range(2)),
                tuple(unit_y * inner[t][n] - edge_y[t][n] for n in range(2)),
                tuple(outer[t][n] - edge_outer[t][n] for n in range(2)),
            ]
        )
    if has_middle:
        square = jnp.where(middle, 1.0 - unit_y * unit_y, 0.0)
        alone = even_part(x, keep * square, mutual * square, decay)
        keep_m, mutual_m = jnp.where(middle, keep_y, 0.0), jnp.where(middle, mutual_y, 0.0)
        cross_x = even_part(x, keep_m, mutual_m, edge_decay)
        cross_y = even_part(y, keep_m, mutual_m, edge_decay)
        for t in range(count):
            out[t][0] = tuple(
                out[t][0][n] + alone[t][n] - cross_x[t][n] - cross_y[t][n] for n in range(2)
            )
            out[t][1] = tuple(out[t][1][n] - cross_x[t][n] for n in range(2))
    return out


def add(a, b):
    return a[0] + b[0], a[1] + b[1]


def sub(a, b):
    return a[0] - b[0], a[1] - b[1]


def add_turned(a, b):
    return a[0] - b[1], a[1] + b[0]


def sub_turned(a, b):
    return a[0] + b[1], a[1] - b[0]


def four_point(z):
    s, d, u, v = add(z[0], z[2]), sub(z[0], z[2]), add(z[1], z[3]), sub(z[1], z[3])
    return add(s, u), sub_turned(d, v), sub(s, u), add_turned(d, v)


def four_point_back(z):
    s, d, u, v = add(z[0], z[2]), sub(z[0], z[2]), add(z[1], z[3]), sub(z[1], z[3])
    return add(s, u), add_turned(d, v), sub(s, u), sub_turned(d, v)


def spread(z):
    turned = [
        z[0],
        (root_half * (z[1][0] + z[1][1]), root_half * (z[1][1] - z[1][0])),
        (z[2][1], -z[2][0]),
        (root_half * (z[3][1] - z[3][0]), -root_half * (z[3][0] + z[3][1])),
    ]
    even, odd = four_point(z), four_point(turned)
    return [even[r // 2] if r % 2 == 0 else odd[r // 2] for r in range(8)]


def gather_back(v):
    even, odd = four_point_back(v[0::2]), four_point_back(v[1::2])
    return [
        add(even[0], odd[0]),
        (even[1][0] + root_half * (odd[1][0] - odd[1][1]), even[1][1] + root_half * (odd[1][0] + odd[1][1])),
        add_turned(even[2], odd[2]),
        (even[3][0] - root_half * (odd[3][0] + odd[3][1]), even[3][1] + root_half * (odd[3][0] - odd[3][1])),
    ]


def middle_kernel(
    rows_ref, coef_ref, edge_ref, sign_ref, twiddle_ref, forward_ref, back_ref, out_ref, work_ref, *, layers
):
    radix = twiddle_ref.shape[1]
    pieces = radix // 2
    steps = rows_ref.shape[1] // sublanes
    items = layers * 3
    place = lax.broadcasted_iota(jnp.int32, (sublanes, lanes), 1)
    low = place < half
    dims = ((1,), (0,))
    forward = (forward_ref[0], forward_ref[1])
    back = (back_ref[0], back_ref[1])

    def run(step, carry):
        here = pl.ds(pl.multiple_of(step * sublanes, sublanes), sublanes)

        def piece(row, part):
            tile, upper = divmod(part, 2)
            cut = slice(tile * lanes, (tile + 1) * lanes)
            first, second = rows_ref[row, here, cut], rows_ref[row + layers, here, cut]
            if upper:
                return jnp.where(low, pltpu.roll(first, half, 1), second)
            return jnp.where(low, first, pltpu.roll(second, half, 1))

        for item in range(items):
            layer, c = divmod(item, 3)
            rows = [2 * p * layers + layer for p in range(pieces)]
            z = [(piece(row, c), piece(row, 3 + c)) for row in rows]
            for r, (real, imag) in enumerate(spread(z)):
                if r > 0:
                    cosine, sine = twiddle_ref[0, r], twiddle_ref[1, r]
                    real, imag = real * cosine + imag * sine, imag * cosine - real * sine
                start = item * sublanes
                work_ref[r, start : start + sublanes, :lanes] = real
                work_ref[r, start : start + sublanes, lanes:] = imag
        for r in range(radix):
            work_ref[r] = product(split(work_ref[r]), forward, dims)
        for r in range(radix):
            value = work_ref[r]
            cuts = [slice(item * sublanes, (item + 1) * sublanes) for item in range(items)]
            pairs = [(value[cut, :lanes], value[cut, lanes:]) for cut in cuts]
            spectrum = [pairs[3 * t : 3 * t + 3] for t in range(layers)]
            coef = [coef_ref[n, r, here] for n in range(coef_count)]
            coef += [edge_ref[n, r : r + 1] for n in range(coef_count)] + [sign_ref[here]]
            out = respond(spectrum, coef, r == 0, place * radix + r == radix * half)
            work_ref[r] = jnp.concatenate(
                [jnp.concatenate([pair[0], pair[1]], axis=1) for layer in out for pair in layer]
            )
        for r in range(radix):
            work_ref[r] = product(split(work_ref[r]), back, dims)
        for layer in range(layers):
            parts = [[None] * 6 for _ in range(pieces)]
            for c in range(3):
                start = (layer * 3 + c) * sublanes
                v = []
                for r in range(radix):
                    real = work_ref[r, start : start + sublanes, :lanes]
                    imag = work_ref[r, start : start + sublanes, lanes:]
                    if r > 0:
                        cosine, sine = twiddle_ref[0, r], twiddle_ref[1, r]
                        real, imag = real * cosine - imag * sine, imag * cosine + real * sine
                    v.append((real, imag))
                for p, (real, imag) in enumerate(gather_back(v)):
                    parts[p][c], parts[p][3 + c] = real, imag
            for p in range(pieces):
                row = 2 * p * layers + layer
                for tile in range(3):
                    first, second = parts[p][2 * tile], parts[p][2 * tile + 1]
                    cut = slice(tile * lanes, (tile + 1) * lanes)
                    out_ref[row, here, cut] = jnp.where(low, first, pltpu.roll(second, half, 1))
                    out_ref[row + layers, here, cut] = jnp.where(low, pltpu.roll(first, half, 1), second)
        return carry

    lax.fori_loop(0, steps, run, 0)


def exchange_kernel(link_ref, moment_ref, below_ref, above_ref, before_ref, after_ref, anisotropy_ref, out_ref):
    rows, cell_count = anisotropy_ref.shape
    row = lax.broadcasted_iota(jnp.int32, (rows, cell_count), 0)
    column = lax.broadcasted_iota(jnp.int32, (rows, cell_count), 1)
    stiffness, lower_link, upper_link = link_ref[0], link_ref[1], link_ref[2]
    for c in range(3):
        m = moment_ref[c]
        before = jnp.where(row == 0, before_ref[c : c + 1], pltpu.roll(m, 1, 0))
        after = jnp.where(row == rows - 1, after_ref[c : c + 1], pltpu.roll(m, rows - 1, 0))
        left = jnp.where(column == 0, 0.0, pltpu.roll(m, 1, 1))
        right = jnp.where(column == cell_count - 1, 0.0, pltpu.roll(m, cell_count - 1, 1))
        total = stiffness * (before + after + left + right)
        total = total + lower_link * below_ref[c] + upper_link * above_ref[c]
        if c == 2:
            total = total + anisotropy_ref[...] * m
        out_ref[c] = total


def last_kernel(
    moment_ref, other_ref, edge_ref, back_ref, twiddle_ref, block_ref, field_hbm, out_hbm,
    field_ref, out_ref, field_sem, out_sem,
):
    rows = moment_ref.shape[1]
    turned = block_ref[...].T
    dims = ((1,), (0,))
    waves = []
    for g in range(4):
        cut = slice(g * lanes, (g + 1) * lanes)
        value = jnp.concatenate([turned[: 3 * rows, cut], turned[3 * rows :, cut]], axis=1)
        table_ref = edge_ref if g == 0 else back_ref
        value = product(split(value), (table_ref[0], table_ref[1]), dims)
        real, imag = value[:, :lanes], value[:, lanes:]
        if g > 0:
            cosine, sine = twiddle_ref[0, g, :1], twiddle_ref[1, g, :1]
            real, imag = real * cosine - imag * sine, imag * cosine + real * sine
        waves.append((real, imag))
    even, odd = waves[0][0] + waves[0][1], waves[0][0] - waves[0][1]
    (real_1, imag_1), (real_2, imag_2), (real_3, imag_3) = waves[1:]
    flat, tilted = root_half * (real_1 - real_3), root_half * (imag_1 + imag_3)
    demag = jnp.concatenate(
        [
            even + real_1 + real_2 + real_3,
            odd + flat - tilted - imag_2,
            even - imag_1 - real_2 + imag_3,
            odd - flat - tilted + imag_2,
        ],
        axis=1,
    )
    for c in range(3):
        field_ref[c] = other_ref[c] + demag[c * rows : (c + 1) * rows]
    sends = [pltpu.make_async_copy(field_ref, field_hbm, field_sem)]
    sends[0].start()
    span = rows // piece_count
    for n in range(piece_count):
        cut = pl.ds(n * span, span)
        m = [moment_ref[c, cut] for c in range(3)]
        first = cross(m, [field_ref[c, cut] for c in range(3)])
        second = cross(m, first)
        stepped = []
        for c in range(3):
            torque = -(first[c] + damping * second[c]) / (1.0 + damping * damping)
            stepped.append(m[c] + time_step * torque)
        scale = lax.rsqrt(stepped[0] * stepped[0] + stepped[1] * stepped[1] + stepped[2] * stepped[2])
        for c in range(3):
            out_ref[c, cut] = stepped[c] * scale
        sends.append(pltpu.make_async_copy(out_ref.at[:, cut], out_hbm.at[:, cut], out_sem.at[n]))
        sends[-1].start()
    for copy in sends:
        copy.wait()


def cross(first, second):
    return [
        first[1] * second[2] - first[2] * second[1],
        first[2] * second[0] - first[0] * second[2],
        first[0] * second[1] - first[1] * second[0],
    ]


def shift(value, axis, step):
    count = lax.axis_size(axis)
    pairs = [(i, i + step) for i in range(count) if 0 <= i + step < count]
    return lax.ppermute(value, axis, pairs)


def fast_body(polar, azimuth, saturation, anisotropy, stiffness, coupling):
    rows, cell_count = polar.shape[1:]
    layers, planes = lax.axis_size("layer"), lax.axis_size("plane")
    device_count = layers * planes
    layer_index = lax.axis_index("layer")
    plane_index = lax.axis_index("plane")
    slots = cell_count // device_count
    radix = 2 * cell_count // lanes
    width = 6 * rows
    f32, bf16 = jnp.float32, jnp.bfloat16
    edge = jnp.asarray(edge_table())
    forward, back = (jnp.asarray(t) for t in short_tables())
    twiddle = jnp.asarray(twiddle_table(radix))
    field_shape = jax.ShapeDtypeStruct((3, rows, cell_count), f32)
    side_shape = (2, sublanes, cell_count)
    block_shape = jax.ShapeDtypeStruct((cell_count, width), f32)
    small = pltpu.CompilerParams(vmem_limit_bytes=vmem_limit)
    dma = pltpu.SemaphoreType.DMA
    flops = 12 * rows * cell_count * cell_count * 6

    moment, side, block = pl.pallas_call(
        first_kernel,
        out_shape=[field_shape, jax.ShapeDtypeStruct(side_shape, f32), block_shape],
        in_specs=[in_any] * 6,
        out_specs=[in_any] * 3,
        scratch_shapes=[
            pltpu.VMEM((3, rows, cell_count), f32),
            pltpu.VMEM(edge.shape, bf16),
            pltpu.VMEM(back.shape, bf16),
            pltpu.VMEM(twiddle.shape, f32),
            pltpu.VMEM((3, rows, cell_count), f32),
            pltpu.VMEM(side_shape, f32),
            pltpu.VMEM((cell_count, width), f32),
            dma((6,)),
            dma((6,)),
        ],
        cost_estimate=pl.CostEstimate(flops=flops, bytes_accessed=4 << 20, transcendentals=0),
        name="first",
    )(polar[0], azimuth[0], saturation[0], edge, back, twiddle)

    base = (plane_index * layers + layer_index).astype(jnp.int32).reshape(1)
    tables = (twiddle, forward, back)
    *coefs, twiddle, forward, back = pl.pallas_call(
        functools.partial(coef_kernel, cell_count=cell_count),
        out_shape=[
            jax.ShapeDtypeStruct((coef_count, radix, slots, lanes), f32),
            jax.ShapeDtypeStruct((coef_count, radix, lanes), f32),
            jax.ShapeDtypeStruct((slots, lanes), f32),
        ]
        + [jax.ShapeDtypeStruct(t.shape, t.dtype) for t in tables],
        in_specs=[in_smem] + [in_vmem] * len(tables),
        out_specs=[in_vmem] * (3 + len(tables)),
        compiler_params=small,
        cost_estimate=pl.CostEstimate(flops=20 << 20, bytes_accessed=1 << 20, transcendentals=1 << 16),
        name="coefs",
    )(base, *tables)

    below = shift(moment, "layer", 1)
    above = shift(moment, "layer", -1)
    before = shift(side[1], "plane", 1)
    after = shift(side[0], "plane", -1)
    links = jnp.stack(
        [
            stiffness[0],
            coupling[jnp.maximum(layer_index - 1, 0)],
            coupling[jnp.minimum(layer_index, coupling.shape[0] - 1)],
        ]
    )
    other = pl.pallas_call(
        exchange_kernel,
        out_shape=field_shape,
        in_specs=[in_smem] + [in_vmem] * 6,
        out_specs=in_vmem,
        compiler_params=small,
        cost_estimate=pl.CostEstimate(flops=20 << 20, bytes_accessed=2 << 20, transcendentals=0),
        name="exchange",
    )(links, moment, below, above, before, after, anisotropy[0])

    exchange_all = functools.partial(
        lax.all_to_all, axis_name=both, split_axis=0, concat_axis=0, tiled=True
    )
    block = exchange_all(block.reshape(device_count, slots, width))
    block, other = lax.optimization_barrier((block, other))
    block = pl.pallas_call(
        functools.partial(middle_kernel, layers=layers),
        out_shape=jax.ShapeDtypeStruct((device_count, slots, width), f32),
        in_specs=[in_vmem] * 7,
        out_specs=in_vmem,
        scratch_shapes=[pltpu.VMEM((radix, layers * 3 * sublanes, 2 * lanes), f32)],
        compiler_params=small,
        cost_estimate=pl.CostEstimate(flops=2000 << 20, bytes_accessed=4 << 20, transcendentals=0),
        name="middle",
    )(block, *coefs, twiddle, forward, back)
    block = exchange_all(block)

    field, stepped = pl.pallas_call(
        last_kernel,
        out_shape=[field_shape] * 2,
        in_specs=[in_vmem] * 6,
        out_specs=[in_any] * 2,
        scratch_shapes=[
            pltpu.VMEM((3, rows, cell_count), f32),
            pltpu.VMEM((3, rows, cell_count), f32),
            dma,
            dma((piece_count,)),
        ],
        compiler_params=small,
        cost_estimate=pl.CostEstimate(flops=flops, bytes_accessed=4 << 20, transcendentals=0),
        name="last",
    )(moment, other, edge, back, twiddle, block.reshape(cell_count, width))
    return field[None], stepped[None]


def with_halo(cells, sides, width):
    for axis, dim in sides:
        count = lax.axis_size(axis)
        ends = count - 1
        head = lax.slice_in_dim(cells, 0, width, axis=dim)
        tail = lax.slice_in_dim(cells, cells.shape[dim] - width, cells.shape[dim], axis=dim)
        cells = jnp.concatenate(
            [
                lax.ppermute(tail, axis, [(i, (i + 1) % count) for i in range(ends)]),
                cells,
                lax.ppermute(head, axis, [((i + 1) % count, i) for i in range(ends)]),
            ],
            axis=dim,
        )
    return cells


def cross_product(first, second):
    return jnp.stack(
        [
            first[1] * second[2] - first[2] * second[1],
            first[2] * second[0] - first[0] * second[2],
            first[0] * second[1] - first[1] * second[0],
        ]
    )


def signed_wave(index, cell_count):
    folded = jnp.where(index < cell_count, index, index - 2 * cell_count)
    return jnp.pi * folded.astype(jnp.float32) / side_length


def plain_body(polar, azimuth, saturation, anisotropy, stiffness, coupling):
    row_count = polar.shape[1]
    cell_count = polar.shape[2]
    pad_length = 2 * cell_count
    plane_count = lax.axis_size("plane")
    band_width = pad_length // plane_count
    layer_index = lax.axis_index("layer")
    plane_index = lax.axis_index("plane")
    theta = polar[0]
    azimuthal = azimuth[0]
    moment_in = jnp.stack(
        [jnp.sin(theta) * jnp.cos(azimuthal), jnp.sin(theta) * jnp.sin(azimuthal), jnp.cos(theta)]
    )
    magnet = moment_in * saturation[0][None]
    place = jnp.arange(cell_count, dtype=jnp.int32)
    wave_index = jnp.arange(pad_length, dtype=jnp.int32)
    turns = place[:, None] * wave_index[None, :] % pad_length
    phase = turns.astype(jnp.float32) * (2.0 * jnp.pi / pad_length)
    cosine = jnp.cos(phase)
    sine = jnp.sin(phase)
    cosine_blocks = cosine.reshape(plane_count, row_count, pad_length)
    sine_blocks = sine.reshape(plane_count, row_count, pad_length)
    cosine_bands = cosine.reshape(cell_count, plane_count, band_width)
    sine_bands = sine.reshape(cell_count, plane_count, band_width)
    along_real = jnp.einsum("cxy,yk->ckx", magnet, cosine, precision=exact)
    along_imag = -jnp.einsum("cxy,yk->ckx", magnet, sine, precision=exact)
    sectioned = jnp.stack([along_real, along_imag], 1).reshape(
        3, 2, plane_count, band_width * row_count
    )
    block = lax.all_to_all(sectioned, "plane", split_axis=2, concat_axis=2, tiled=True)
    item_count = block.shape[0]
    split = block.reshape(item_count, 2, plane_count, band_width, row_count)
    with_cosine = jnp.einsum("npsqx,sxk->npqk", split, cosine_blocks, precision=exact)
    with_sine = jnp.einsum("npsqx,sxk->npqk", split, sine_blocks, precision=exact)
    spectrum = jnp.stack(
        [with_cosine[:, 0] + with_sine[:, 1], with_cosine[:, 1] - with_sine[:, 0]], 1
    )
    wave_y = signed_wave(
        plane_index * band_width + jnp.arange(band_width, dtype=jnp.int32), cell_count
    )[:, None]
    wave_x = signed_wave(wave_index, cell_count)[None, :]
    magnitude = jnp.sqrt(wave_x * wave_x + wave_y * wave_y)
    nonzero = magnitude > 0.0
    safe = jnp.where(nonzero, magnitude, 1.0)
    unit_x = jnp.where(nonzero, wave_x / safe, 0.0)
    unit_y = jnp.where(nonzero, wave_y / safe, 0.0)
    self_part = jnp.where(nonzero, -jnp.expm1(-safe) / safe, 1.0)
    half_sinh = jnp.sinh(0.5 * safe)
    mutual = jnp.where(nonzero, 2.0 * half_sinh * half_sinh / safe, 0.0)
    spectral_x = spectrum[0]
    spectral_y = spectrum[1]
    spectral_z = spectrum[2]
    inplane = unit_x * spectral_x + unit_y * spectral_y
    upward = jnp.stack([spectral_z[0] + inplane[1], spectral_z[1] - inplane[0]])
    downward = jnp.stack([-spectral_z[0] + inplane[1], -spectral_z[1] - inplane[0]])
    emitted = jnp.stack([upward, downward])[None]
    piece = lax.all_gather(emitted, "layer", axis=0, tiled=True)
    source = jnp.arange(piece.shape[0], dtype=jnp.int32)
    separation = layer_index - source
    distance = jnp.abs(separation).astype(jnp.float32)
    weight = jnp.exp(-spacing * distance[:, None, None] * magnitude[None])
    lower = jnp.where((separation > 0)[:, None, None], weight, 0.0)
    upper = jnp.where((separation < 0)[:, None, None], weight, 0.0)
    below = jnp.sum(lower[:, None] * piece[:, 0], 0)
    above = jnp.sum(upper[:, None] * piece[:, 1], 0)
    total = below + above
    differ = below - above
    remainder = 1.0 - self_part
    field_x = jnp.stack(
        [
            -remainder * unit_x * inplane[0] + unit_x * mutual * total[1],
            -remainder * unit_x * inplane[1] - unit_x * mutual * total[0],
        ]
    )
    field_y = jnp.stack(
        [
            -remainder * unit_y * inplane[0] + unit_y * mutual * total[1],
            -remainder * unit_y * inplane[1] - unit_y * mutual * total[0],
        ]
    )
    field_z = jnp.stack(
        [
            -self_part * spectral_z[0] + mutual * differ[0],
            -self_part * spectral_z[1] + mutual * differ[1],
        ]
    )
    spectral = jnp.stack([field_x, field_y, field_z])
    back_cosine = jnp.einsum("cpqk,sxk->cpsqx", spectral, cosine_blocks, precision=exact)
    back_sine = jnp.einsum("cpqk,sxk->cpsqx", spectral, sine_blocks, precision=exact)
    returned = jnp.stack(
        [back_cosine[:, 0] - back_sine[:, 1], back_sine[:, 0] + back_cosine[:, 1]], 1
    )
    returned = returned.reshape(3, 2, plane_count, band_width * row_count)
    scale = 1.0 / (float(pad_length) * float(pad_length))
    block = lax.all_to_all(returned, "plane", split_axis=2, concat_axis=2, tiled=True)
    item_count = block.shape[0]
    split = block.reshape(item_count, 2, plane_count, band_width, row_count)
    real_part = jnp.einsum("nsqx,ysq->nxy", split[:, 0], cosine_bands, precision=exact)
    imag_part = jnp.einsum("nsqx,ysq->nxy", split[:, 1], sine_bands, precision=exact)
    demag = (real_part - imag_part) * scale
    padded = with_halo(moment_in[None], (("layer", 0), ("plane", 2)), 1)
    centre = padded[1]
    beside = centre[:, :-2] + centre[:, 2:]
    sideways = jnp.pad(moment_in, ((0, 0), (0, 0), (1, 1)))
    beside = beside + sideways[:, :, :-2] + sideways[:, :, 2:]
    lower_link = coupling[jnp.maximum(layer_index - 1, 0)]
    upper_link = coupling[jnp.minimum(layer_index, coupling.shape[0] - 1)]
    exchange_field = (
        stiffness[0] * beside + lower_link * padded[0, :, 1:-1] + upper_link * padded[2, :, 1:-1]
    )
    flat_zero = jnp.zeros_like(moment_in[2])
    uniaxial = jnp.stack([flat_zero, flat_zero, anisotropy[0] * moment_in[2]])
    field = demag + exchange_field + uniaxial
    first_cross = cross_product(moment_in, field)
    second_cross = cross_product(moment_in, first_cross)
    torque = -(first_cross + damping * second_cross) / (1.0 + damping * damping)
    stepped = moment_in + time_step * torque
    length = jnp.sqrt(jnp.sum(stepped * stepped, axis=0, keepdims=True))
    return (field[None], (stepped / length)[None])


def body(polar, azimuth, saturation, anisotropy, stiffness, coupling):
    rows, cell_count = polar.shape[1:]
    device_count = lax.axis_size("layer") * lax.axis_size("plane")
    fits = 2 * rows == lanes and cell_count == 4 * lanes
    fits = fits and cell_count % (device_count * sublanes) == 0
    chosen = fast_body if fits else plain_body
    return chosen(polar, azimuth, saturation, anisotropy, stiffness, coupling)


def solution(mesh):
    placed = (
        P("layer", "plane", None),
        P("layer", "plane", None),
        P("layer", "plane", None),
        P("layer", "plane", None),
        P("layer"),
        P(),
    )
    return jax.shard_map(
        body,
        mesh=mesh,
        in_specs=placed,
        out_specs=(P("layer", None, "plane", None), P("layer", None, "plane", None)),
        check_vma=False,
    )
```

```python
import functools
import math

import jax
import jax.numpy as jnp
import numpy as np
from jax import lax
from jax.experimental import pallas as pl
from jax.experimental.pallas import tpu as pltpu
from jax.sharding import PartitionSpec as P


side_length = 512.0
spacing = 1.2
damping = 0.1
time_step = 0.1
exact = lax.Precision.HIGHEST

lanes = 128
sublanes = 8
half = lanes // 2
root_half = math.sqrt(0.5)
piece_count = 2
coef_count = 6
vmem_limit = 16 << 20
both = ("plane", "layer")
in_vmem = pl.BlockSpec(memory_space=pltpu.VMEM)
in_any = pl.BlockSpec(memory_space=pl.ANY)
in_smem = pl.BlockSpec(memory_space=pltpu.SMEM)


def split_table(table):
    head = table.astype(np.float32).astype(jnp.bfloat16)
    rest = (table - head.astype(np.float64)).astype(np.float32).astype(jnp.bfloat16)
    return np.stack([head, rest])


def edge_table():
    slot, place = np.arange(half), np.arange(lanes)
    zero = np.zeros((half, lanes))
    phase = [2.0 * np.pi / (8 * lanes) * (np.outer(8 * slot + r, place) % (8 * lanes)) for r in (0, 4)]
    rows = [np.block([[f(phase[0]), zero], [zero, f(phase[1])]]) for f in (np.cos, np.sin)]
    return split_table(np.concatenate([rows[0], -rows[1]]))


def short_table():
    turns = np.outer(np.arange(lanes), np.arange(lanes)) % lanes
    phase = turns * (2.0 * np.pi / lanes)
    c, s = np.cos(phase), np.sin(phase)
    return split_table(np.block([[c, s], [-s, c]]))


def twiddle_table(radix):
    phase = np.outer(np.arange(radix), np.arange(lanes)) * (2.0 * np.pi / (radix * lanes))
    pair = np.stack([np.cos(phase), np.sin(phase)]).astype(np.float32)
    return np.ascontiguousarray(np.broadcast_to(pair[:, :, None], (2, radix, sublanes, lanes)))


def split(value):
    head = value.astype(jnp.bfloat16)
    return head, (value - head.astype(jnp.float32)).astype(jnp.bfloat16)


def product(left, right, dims):
    (axis,), (other,) = dims
    return lax.dot_general(
        jnp.concatenate([left[0], left[1], left[0]], axis=axis),
        jnp.concatenate([right[0], right[0], right[1]], axis=other),
        dimension_numbers=(dims, ((), ())),
        preferred_element_type=jnp.float32,
    )


def sine_cosine(angle):
    square = angle * angle
    sine = jnp.full_like(angle, 1.0 / math.factorial(13))
    for order in (11, 9, 7, 5, 3, 1):
        sine = (-1.0) ** ((order - 1) // 2) / math.factorial(order) + square * sine
    cosine = jnp.full_like(angle, -1.0 / math.factorial(14))
    for order in (12, 10, 8, 6, 4, 2, 0):
        cosine = (-1.0) ** (order // 2) / math.factorial(order) + square * cosine
    return angle * sine, cosine


def first_kernel(
    polar_hbm, azimuth_hbm, saturation_hbm, edge_hbm, back_hbm, twiddle_hbm, moment_hbm, side_hbm, out_hbm,
    angle_ref, edge_ref, back_ref, twiddle_ref, moment_ref, side_ref, rows_ref, in_sem, out_sem,
):
    rows, _ = angle_ref.shape[1:]
    sources = (polar_hbm, azimuth_hbm, saturation_hbm, edge_hbm, back_hbm, twiddle_hbm)
    places = (angle_ref.at[0], angle_ref.at[1], angle_ref.at[2], edge_ref, back_ref, twiddle_ref)
    loads = [
        pltpu.make_async_copy(source, place, in_sem.at[n])
        for n, (source, place) in enumerate(zip(sources, places))
    ]
    for copy in loads:
        copy.start()
    for copy in loads:
        copy.wait()
    sin_polar, cos_polar = sine_cosine(angle_ref[0])
    sin_half, cos_half = sine_cosine(0.5 * angle_ref[1])
    saturation = angle_ref[2]
    moment = (
        sin_polar * (1.0 - 2.0 * sin_half * sin_half),
        sin_polar * (2.0 * sin_half * cos_half),
        cos_polar,
    )
    groups = [[] for _ in range(4)]
    for c in range(3):
        moment_ref[c] = moment[c]
        side_ref[0, c : c + 1] = moment[c][:1]
        side_ref[1, c : c + 1] = moment[c][rows - 1 :]
        magnet = moment[c] * saturation
        a = [magnet[:, p * lanes : (p + 1) * lanes] for p in range(4)]
        even, odd = a[0] + a[2], a[1] + a[3]
        turned, mixed = root_half * (a[1] - a[3]), root_half * odd
        groups[0].append((even + odd, even - odd))
        for r, (real, imag) in (
            (1, (a[0] + turned, -a[2] - mixed)),
            (2, (a[0] - a[2], a[3] - a[1])),
            (3, (a[0] - turned, a[2] - mixed)),
        ):
            cosine, sine = twiddle_ref[0, r, :1], twiddle_ref[1, r, :1]
            groups[r].append((real * cosine + imag * sine, imag * cosine - real * sine))
    sends = [
        pltpu.make_async_copy(moment_ref, moment_hbm, out_sem.at[0]),
        pltpu.make_async_copy(side_ref, side_hbm, out_sem.at[1]),
    ]
    for copy in sends:
        copy.start()
    blank = jnp.zeros((rows, 2 * lanes), jnp.bfloat16)
    dims = ((1,), (1,))
    for g in range(4):
        parts = [split(jnp.concatenate(pair, axis=1)) for pair in groups[g]]
        for_real = [jnp.concatenate([part[n] for part in parts] + [blank]) for n in range(2)]
        for_imag = [jnp.concatenate([blank] + [part[n] for part in parts]) for n in range(2)]
        table_ref = edge_ref if g == 0 else back_ref
        real = product((table_ref[0, :lanes], table_ref[1, :lanes]), for_real, dims)
        imag = product((table_ref[0, lanes:], table_ref[1, lanes:]), for_imag, dims)
        cut = slice(g * lanes, (g + 1) * lanes)
        rows_ref[cut, :lanes] = real[:, :lanes]
        rows_ref[cut, lanes : 2 * lanes] = real[:, lanes:] + imag[:, :lanes]
        rows_ref[cut, 2 * lanes :] = imag[:, lanes:]
        sends.append(pltpu.make_async_copy(rows_ref.at[cut], out_hbm.at[cut], out_sem.at[2 + g]))
        sends[-1].start()
    for copy in sends:
        copy.wait()


def factors(wave_x, wave_y):
    magnitude = jnp.sqrt(wave_x * wave_x + wave_y * wave_y)
    nonzero = magnitude > 0.0
    safe = jnp.where(nonzero, magnitude, 1.0)
    inverse = 1.0 / safe
    series = jnp.ones_like(safe)
    for order in range(9, 1, -1):
        series = 1.0 - series * safe * (1.0 / order)
    growth = jnp.exp(safe)
    lost = jnp.where(safe < 0.5, series * safe, 1.0 - jnp.exp(-safe))
    self_part = jnp.where(nonzero, lost * inverse, 1.0)
    mutual = jnp.where(nonzero, lost * lost * growth * (0.5 * inverse), 0.0)
    decay = jnp.exp(-spacing * magnitude)
    unit_x = jnp.where(nonzero, wave_x * inverse, 0.0)
    unit_y = jnp.where(nonzero, wave_y * inverse, 0.0)
    return unit_x, unit_y, self_part, mutual, decay


def coef_kernel(base_ref, *refs, cell_count):
    count = len(refs) // 2 - 1
    out_ref, edge_ref, sign_ref = refs[count : count + 3]
    for table_ref, kept_ref in zip(refs[:count], refs[count + 3 :]):
        kept_ref[...] = table_ref[...]
    pad_length = 2 * cell_count
    radix = pad_length // lanes
    step = math.pi / side_length
    slots = out_ref.shape[2]
    shape = (slots, lanes)
    slot = base_ref[0] * slots + lax.broadcasted_iota(jnp.int32, shape, 0)
    group, order = slot // lanes, slot % lanes
    first = jnp.where(order < half, order * radix, (order - half) * radix + radix // 2)
    wave = jnp.where(group == 0, first, order * radix + group)
    wave_y = step * jnp.where(wave < cell_count, wave, wave - pad_length).astype(jnp.float32)
    weight = jnp.where(wave == 0, 1.0, 2.0) / float(pad_length * pad_length)
    sign_ref[...] = jnp.where(wave % 2 == 0, weight, -weight)
    for r in range(radix):
        index = lax.broadcasted_iota(jnp.int32, shape, 1) * radix + r
        folded = jnp.where(index < cell_count, index, index - pad_length)
        unit_x, unit_y, self_part, mutual, decay = factors(step * folded.astype(jnp.float32), wave_y)
        out_ref[0, r] = jnp.where(index == cell_count, 0.0, unit_x)
        out_ref[1, r] = unit_y
        out_ref[2, r] = (1.0 - self_part) * weight
        out_ref[3, r] = self_part * weight
        out_ref[4, r] = mutual * weight
        out_ref[5, r] = decay
    shape = (radix, lanes)
    index = lax.broadcasted_iota(jnp.int32, shape, 1) * radix + lax.broadcasted_iota(jnp.int32, shape, 0)
    folded = jnp.where(index < cell_count, index, index - pad_length)
    wave_y = jnp.full(shape, -step * cell_count, jnp.float32)
    edge_x, edge_y, self_part, mutual, decay = factors(step * folded.astype(jnp.float32), wave_y)
    edge_ref[0] = jnp.where(index == cell_count, 0.0, edge_x)
    edge_ref[1] = 1.0 - self_part
    edge_ref[2] = self_part
    edge_ref[3] = mutual
    edge_ref[4] = decay
    edge_ref[5] = edge_y * edge_y


def neighbours(values, decay):
    count = len(values)
    under = [None] * count
    over = [None] * count
    for t in range(1, count):
        under[t] = decay * (values[t - 1] if under[t - 1] is None else under[t - 1] + values[t - 1])
    for t in range(count - 2, -1, -1):
        over[t] = decay * (values[t + 1] if over[t + 1] is None else over[t + 1] + values[t + 1])
    return under, over


def joined(first, second, sign=1.0):
    if first is None:
        return second if sign > 0.0 else -second
    if second is None:
        return first
    return first + second if sign > 0.0 else first - second


def drive(x, z, keep, mutual, decay, own):
    count = len(x)
    up_r, over_r = [z[t][0] + x[t][1] for t in range(count)], [x[t][1] - z[t][0] for t in range(count)]
    up_i, over_i = [z[t][1] - x[t][0] for t in range(count)], [-z[t][1] - x[t][0] for t in range(count)]
    below_r, below_i = neighbours(up_r, decay)[0], neighbours(up_i, decay)[0]
    above_r, above_i = neighbours(over_r, decay)[1], neighbours(over_i, decay)[1]
    inner, outer = [], []
    for t in range(count):
        total_r, total_i = joined(below_r[t], above_r[t]), joined(below_i[t], above_i[t])
        differ_r = joined(below_r[t], above_r[t], -1.0)
        differ_i = joined(below_i[t], above_i[t], -1.0)
        inner.append((mutual * total_i - keep * x[t][0], -(mutual * total_r) - keep * x[t][1]))
        outer.append((mutual * differ_r - own * z[t][0], mutual * differ_i - own * z[t][1]))
    return inner, outer


def even_part(values, keep, mutual, decay):
    out = []
    for n in range(2):
        part = [v[n] for v in values]
        under, over = neighbours(part, decay)
        out.append([-(keep * part[t]) - mutual * joined(under[t], over[t]) for t in range(len(part))])
    return list(zip(*out))


def respond(spectrum, coef, has_middle, middle):
    count = len(spectrum)
    unit_x, unit_y, keep, own, mutual, decay = coef[:6]
    edge_x, edge_keep, edge_own, edge_mutual, edge_decay, square_y, sign = coef[6:]
    edge_keep, edge_own, edge_mutual = sign * edge_keep, sign * edge_own, sign * edge_mutual
    keep_y, mutual_y = square_y * edge_keep, square_y * edge_mutual
    x = [s[0] for s in spectrum]
    y = [s[1] for s in spectrum]
    z = [s[2] for s in spectrum]
    charge = [tuple(unit_x * x[t][n] + unit_y * y[t][n] for n in range(2)) for t in range(count)]
    inner, outer = drive(charge, z, keep, mutual, decay, own)
    charge = [tuple(edge_x * x[t][n] for n in range(2)) for t in range(count)]
    edge_inner, edge_outer = drive(charge, z, edge_keep, edge_mutual, edge_decay, edge_own)
    edge_y = even_part(y, keep_y, mutual_y, edge_decay)
    out = []
    for t in range(count):
        out.append(
            [
                tuple(unit_x * inner[t][n] - edge_x * edge_inner[t][n] for n in range(2)),
                tuple(unit_y * inner[t][n] - edge_y[t][n] for n in range(2)),
                tuple(outer[t][n] - edge_outer[t][n] for n in range(2)),
            ]
        )
    if has_middle:
        square = jnp.where(middle, 1.0 - unit_y * unit_y, 0.0)
        alone = even_part(x, keep * square, mutual * square, decay)
        keep_m, mutual_m = jnp.where(middle, keep_y, 0.0), jnp.where(middle, mutual_y, 0.0)
        cross_x = even_part(x, keep_m, mutual_m, edge_decay)
        cross_y = even_part(y, keep_m, mutual_m, edge_decay)
        for t in range(count):
            out[t][0] = tuple(
                out[t][0][n] + alone[t][n] - cross_x[t][n] - cross_y[t][n] for n in range(2)
            )
            out[t][1] = tuple(out[t][1][n] - cross_x[t][n] for n in range(2))
    return out


def add(a, b):
    return a[0] + b[0], a[1] + b[1]


def sub(a, b):
    return a[0] - b[0], a[1] - b[1]


def add_turned(a, b):
    return a[0] - b[1], a[1] + b[0]


def sub_turned(a, b):
    return a[0] + b[1], a[1] - b[0]


def four_point(z):
    s, d, u, v = add(z[0], z[2]), sub(z[0], z[2]), add(z[1], z[3]), sub(z[1], z[3])
    return add(s, u), sub_turned(d, v), sub(s, u), add_turned(d, v)


def four_point_back(z):
    s, d, u, v = add(z[0], z[2]), sub(z[0], z[2]), add(z[1], z[3]), sub(z[1], z[3])
    return add(s, u), add_turned(d, v), sub(s, u), sub_turned(d, v)


def spread(z):
    turned = [
        z[0],
        (root_half * (z[1][0] + z[1][1]), root_half * (z[1][1] - z[1][0])),
        (z[2][1], -z[2][0]),
        (root_half * (z[3][1] - z[3][0]), -root_half * (z[3][0] + z[3][1])),
    ]
    even, odd = four_point(z), four_point(turned)
    return [even[r // 2] if r % 2 == 0 else odd[r // 2] for r in range(8)]


def gather_back(v):
    even, odd = four_point_back(v[0::2]), four_point_back(v[1::2])
    return [
        add(even[0], odd[0]),
        (even[1][0] + root_half * (odd[1][0] - odd[1][1]), even[1][1] + root_half * (odd[1][0] + odd[1][1])),
        add_turned(even[2], odd[2]),
        (even[3][0] - root_half * (odd[3][0] + odd[3][1]), even[3][1] + root_half * (odd[3][0] - odd[3][1])),
    ]


def middle_kernel(
    rows_ref, coef_ref, edge_ref, sign_ref, twiddle_ref, back_ref, out_ref, work_ref, *, layers
):
    radix = twiddle_ref.shape[1]
    pieces = radix // 2
    steps = rows_ref.shape[1] // sublanes
    items = layers * 3
    place = lax.broadcasted_iota(jnp.int32, (sublanes, lanes), 1)
    low = place < half
    dims = ((1,), (0,))
    back = (back_ref[0], back_ref[1])
    upper = [jnp.concatenate([b[:lanes, :lanes], b[lanes:, :lanes]], axis=1) for b in back]
    lower = [jnp.concatenate([b[:lanes, lanes:], b[lanes:, lanes:]], axis=1) for b in back]
    forward = tuple(jnp.concatenate(pair) for pair in zip(upper, lower))

    def run(step, carry):
        here = pl.ds(pl.multiple_of(step * sublanes, sublanes), sublanes)

        def piece(row, part):
            tile, upper = divmod(part, 2)
            cut = slice(tile * lanes, (tile + 1) * lanes)
            first, second = rows_ref[row, here, cut], rows_ref[row + layers, here, cut]
            if upper:
                return jnp.where(low, pltpu.roll(first, half, 1), second)
            return jnp.where(low, first, pltpu.roll(second, half, 1))

        for item in range(items):
            layer, c = divmod(item, 3)
            rows = [2 * p * layers + layer for p in range(pieces)]
            z = [(piece(row, c), piece(row, 3 + c)) for row in rows]
            for r, (real, imag) in enumerate(spread(z)):
                if r > 0:
                    cosine, sine = twiddle_ref[0, r], twiddle_ref[1, r]
                    real, imag = real * cosine + imag * sine, imag * cosine - real * sine
                start = item * sublanes
                work_ref[r, start : start + sublanes, :lanes] = real
                work_ref[r, start : start + sublanes, lanes:] = imag
        for r in range(radix):
            work_ref[r] = product(split(work_ref[r]), forward, dims)
        for r in range(radix):
            value = work_ref[r]
            cuts = [slice(item * sublanes, (item + 1) * sublanes) for item in range(items)]
            pairs = [(value[cut, :lanes], value[cut, lanes:]) for cut in cuts]
            spectrum = [pairs[3 * t : 3 * t + 3] for t in range(layers)]
            coef = [coef_ref[n, r, here] for n in range(coef_count)]
            coef += [edge_ref[n, r : r + 1] for n in range(coef_count)] + [sign_ref[here]]
            out = respond(spectrum, coef, r == 0, place * radix + r == radix * half)
            work_ref[r] = jnp.concatenate(
                [jnp.concatenate([pair[0], pair[1]], axis=1) for layer in out for pair in layer]
            )
        for r in range(radix):
            work_ref[r] = product(split(work_ref[r]), back, dims)
        for layer in range(layers):
            parts = [[None] * 6 for _ in range(pieces)]
            for c in range(3):
                start = (layer * 3 + c) * sublanes
                v = []
                for r in range(radix):
                    real = work_ref[r, start : start + sublanes, :lanes]
                    imag = work_ref[r, start : start + sublanes, lanes:]
                    if r > 0:
                        cosine, sine = twiddle_ref[0, r], twiddle_ref[1, r]
                        real, imag = real * cosine - imag * sine, imag * cosine + real * sine
                    v.append((real, imag))
                for p, (real, imag) in enumerate(gather_back(v)):
                    parts[p][c], parts[p][3 + c] = real, imag
            for p in range(pieces):
                row = 2 * p * layers + layer
                for tile in range(3):
                    first, second = parts[p][2 * tile], parts[p][2 * tile + 1]
                    cut = slice(tile * lanes, (tile + 1) * lanes)
                    out_ref[row, here, cut] = jnp.where(low, first, pltpu.roll(second, half, 1))
                    out_ref[row + layers, here, cut] = jnp.where(low, pltpu.roll(first, half, 1), second)
        return carry

    lax.fori_loop(0, steps, run, 0)


def exchange_kernel(place_ref, stiffness_ref, coupling_ref, moment_ref, below_ref, above_ref, anisotropy_ref, out_ref, scale_ref):
    scale_ref[...] = jnp.full_like(scale_ref, stiffness_ref[0])
    rows, cell_count = anisotropy_ref.shape
    row = lax.broadcasted_iota(jnp.int32, (rows, cell_count), 0)
    column = lax.broadcasted_iota(jnp.int32, (rows, cell_count), 1)
    stiffness = stiffness_ref[0]
    lower_link = coupling_ref[jnp.maximum(place_ref[1] - 1, 0)]
    upper_link = coupling_ref[jnp.minimum(place_ref[1], coupling_ref.shape[0] - 1)]
    for c in range(3):
        m = moment_ref[c]
        before = jnp.where(row == 0, 0.0, pltpu.roll(m, 1, 0))
        after = jnp.where(row == rows - 1, 0.0, pltpu.roll(m, rows - 1, 0))
        left = jnp.where(column == 0, 0.0, pltpu.roll(m, 1, 1))
        right = jnp.where(column == cell_count - 1, 0.0, pltpu.roll(m, cell_count - 1, 1))
        total = stiffness * (before + after + left + right)
        total = total + lower_link * below_ref[c] + upper_link * above_ref[c]
        if c == 2:
            total = total + anisotropy_ref[...] * m
        out_ref[c] = total


def last_kernel(
    before_any, after_any, scale_any, moment_ref, other_ref, edge_ref, back_ref, twiddle_ref, block_ref,
    field_hbm, out_hbm, field_ref, out_ref, side_ref, field_sem, out_sem, side_sem,
):
    rows = moment_ref.shape[1]
    sides = [
        pltpu.make_async_copy(source, side_ref.at[n], side_sem.at[n])
        for n, source in enumerate((before_any, after_any, scale_any))
    ]
    for copy in sides:
        copy.start()
    turned = block_ref[...].T
    dims = ((1,), (0,))
    waves = []
    for g in range(4):
        cut = slice(g * lanes, (g + 1) * lanes)
        value = jnp.concatenate([turned[: 3 * rows, cut], turned[3 * rows :, cut]], axis=1)
        table_ref = edge_ref if g == 0 else back_ref
        value = product(split(value), (table_ref[0], table_ref[1]), dims)
        real, imag = value[:, :lanes], value[:, lanes:]
        if g > 0:
            cosine, sine = twiddle_ref[0, g, :1], twiddle_ref[1, g, :1]
            real, imag = real * cosine - imag * sine, imag * cosine + real * sine
        waves.append((real, imag))
    even, odd = waves[0][0] + waves[0][1], waves[0][0] - waves[0][1]
    (real_1, imag_1), (real_2, imag_2), (real_3, imag_3) = waves[1:]
    flat, tilted = root_half * (real_1 - real_3), root_half * (imag_1 + imag_3)
    demag = jnp.concatenate(
        [
            even + real_1 + real_2 + real_3,
            odd + flat - tilted - imag_2,
            even - imag_1 - real_2 + imag_3,
            odd - flat - tilted + imag_2,
        ],
        axis=1,
    )
    for copy in sides:
        copy.wait()
    for c in range(3):
        field_ref[c] = other_ref[c] + demag[c * rows : (c + 1) * rows]
        field_ref[c, :1] += side_ref[2, :1] * side_ref[0, c : c + 1]
        field_ref[c, rows - 1 :] += side_ref[2, :1] * side_ref[1, c : c + 1]
    sends = [pltpu.make_async_copy(field_ref, field_hbm, field_sem)]
    sends[0].start()
    span = rows // piece_count
    for n in range(piece_count):
        cut = pl.ds(n * span, span)
        m = [moment_ref[c, cut] for c in range(3)]
        first = cross(m, [field_ref[c, cut] for c in range(3)])
        second = cross(m, first)
        stepped = []
        for c in range(3):
            torque = -(first[c] + damping * second[c]) / (1.0 + damping * damping)
            stepped.append(m[c] + time_step * torque)
        scale = lax.rsqrt(stepped[0] * stepped[0] + stepped[1] * stepped[1] + stepped[2] * stepped[2])
        for c in range(3):
            out_ref[c, cut] = stepped[c] * scale
        sends.append(pltpu.make_async_copy(out_ref.at[:, cut], out_hbm.at[:, cut], out_sem.at[n]))
        sends[-1].start()
    for copy in sends:
        copy.wait()


def cross(first, second):
    return [
        first[1] * second[2] - first[2] * second[1],
        first[2] * second[0] - first[0] * second[2],
        first[0] * second[1] - first[1] * second[0],
    ]


def shift(value, axis, step):
    count = lax.axis_size(axis)
    pairs = [(i, i + step) for i in range(count) if 0 <= i + step < count]
    return lax.ppermute(value, axis, pairs)


def fast_body(polar, azimuth, saturation, anisotropy, stiffness, coupling):
    rows, cell_count = polar.shape[1:]
    layers, planes = lax.axis_size("layer"), lax.axis_size("plane")
    device_count = layers * planes
    layer_index = lax.axis_index("layer")
    plane_index = lax.axis_index("plane")
    slots = cell_count // device_count
    radix = 2 * cell_count // lanes
    width = 6 * rows
    f32, bf16 = jnp.float32, jnp.bfloat16
    edge = jnp.asarray(edge_table())
    back = jnp.asarray(short_table())
    twiddle = jnp.asarray(twiddle_table(radix))
    field_shape = jax.ShapeDtypeStruct((3, rows, cell_count), f32)
    side_shape = (2, sublanes, cell_count)
    block_shape = jax.ShapeDtypeStruct((cell_count, width), f32)
    small = pltpu.CompilerParams(vmem_limit_bytes=vmem_limit)
    dma = pltpu.SemaphoreType.DMA
    flops = 12 * rows * cell_count * cell_count * 6

    moment, side, block = pl.pallas_call(
        first_kernel,
        out_shape=[field_shape, jax.ShapeDtypeStruct(side_shape, f32), block_shape],
        in_specs=[in_any] * 6,
        out_specs=[in_any] * 3,
        scratch_shapes=[
            pltpu.VMEM((3, rows, cell_count), f32),
            pltpu.VMEM(edge.shape, bf16),
            pltpu.VMEM(back.shape, bf16),
            pltpu.VMEM(twiddle.shape, f32),
            pltpu.VMEM((3, rows, cell_count), f32),
            pltpu.VMEM(side_shape, f32),
            pltpu.VMEM((cell_count, width), f32),
            dma((6,)),
            dma((6,)),
        ],
        cost_estimate=pl.CostEstimate(flops=flops, bytes_accessed=4 << 20, transcendentals=0),
        name="first",
    )(polar[0], azimuth[0], saturation[0], edge, back, twiddle)

    base = jnp.stack([plane_index * layers + layer_index, layer_index]).astype(jnp.int32)
    tables = (twiddle, back)
    *coefs, kept_twiddle, kept_back = pl.pallas_call(
        functools.partial(coef_kernel, cell_count=cell_count),
        out_shape=[
            jax.ShapeDtypeStruct((coef_count, radix, slots, lanes), f32),
            jax.ShapeDtypeStruct((coef_count, radix, lanes), f32),
            jax.ShapeDtypeStruct((slots, lanes), f32),
        ]
        + [jax.ShapeDtypeStruct(t.shape, t.dtype) for t in tables],
        in_specs=[in_smem] + [in_vmem] * len(tables),
        out_specs=[in_vmem] * (3 + len(tables)),
        compiler_params=small,
        cost_estimate=pl.CostEstimate(flops=20 << 20, bytes_accessed=1 << 20, transcendentals=1 << 16),
        name="coefs",
    )(base, *tables)

    below = shift(moment, "layer", 1)
    above = shift(moment, "layer", -1)
    before = shift(side[1], "plane", 1)
    after = shift(side[0], "plane", -1)
    other, scale = pl.pallas_call(
        exchange_kernel,
        out_shape=[field_shape, jax.ShapeDtypeStruct(side_shape[1:], f32)],
        in_specs=[in_smem] * 3 + [in_vmem] * 4,
        out_specs=[in_vmem] * 2,
        compiler_params=small,
        cost_estimate=pl.CostEstimate(flops=20 << 20, bytes_accessed=2 << 20, transcendentals=0),
        name="exchange",
    )(base, stiffness, coupling, moment, below, above, anisotropy[0])

    exchange_all = functools.partial(
        lax.all_to_all, axis_name=both, split_axis=0, concat_axis=0, tiled=True
    )
    block = exchange_all(block.reshape(device_count, slots, width))
    block, other = lax.optimization_barrier((block, other))
    block = pl.pallas_call(
        functools.partial(middle_kernel, layers=layers),
        out_shape=jax.ShapeDtypeStruct((device_count, slots, width), f32),
        in_specs=[in_vmem] * 6,
        out_specs=in_vmem,
        scratch_shapes=[pltpu.VMEM((radix, layers * 3 * sublanes, 2 * lanes), f32)],
        compiler_params=small,
        cost_estimate=pl.CostEstimate(flops=2000 << 20, bytes_accessed=4 << 20, transcendentals=0),
        name="middle",
    )(block, *coefs, kept_twiddle, kept_back)
    block, before, after = lax.optimization_barrier((block, before, after))
    block = exchange_all(block)

    field, stepped = pl.pallas_call(
        last_kernel,
        out_shape=[field_shape] * 2,
        in_specs=[in_any] * 3 + [in_vmem] * 6,
        out_specs=[in_any] * 2,
        scratch_shapes=[
            pltpu.VMEM((3, rows, cell_count), f32),
            pltpu.VMEM((3, rows, cell_count), f32),
            pltpu.VMEM((3, *side_shape[1:]), f32),
            dma,
            dma((piece_count,)),
            dma((3,)),
        ],
        compiler_params=small,
        cost_estimate=pl.CostEstimate(flops=flops, bytes_accessed=4 << 20, transcendentals=0),
        name="last",
    )(before, after, scale, moment, other, edge, back, twiddle, block.reshape(cell_count, width))
    return field[None], stepped[None]


def with_halo(cells, sides, width):
    for axis, dim in sides:
        count = lax.axis_size(axis)
        ends = count - 1
        head = lax.slice_in_dim(cells, 0, width, axis=dim)
        tail = lax.slice_in_dim(cells, cells.shape[dim] - width, cells.shape[dim], axis=dim)
        cells = jnp.concatenate(
            [
                lax.ppermute(tail, axis, [(i, (i + 1) % count) for i in range(ends)]),
                cells,
                lax.ppermute(head, axis, [((i + 1) % count, i) for i in range(ends)]),
            ],
            axis=dim,
        )
    return cells


def cross_product(first, second):
    return jnp.stack(
        [
            first[1] * second[2] - first[2] * second[1],
            first[2] * second[0] - first[0] * second[2],
            first[0] * second[1] - first[1] * second[0],
        ]
    )


def signed_wave(index, cell_count):
    folded = jnp.where(index < cell_count, index, index - 2 * cell_count)
    return jnp.pi * folded.astype(jnp.float32) / side_length


def plain_body(polar, azimuth, saturation, anisotropy, stiffness, coupling):
    row_count = polar.shape[1]
    cell_count = polar.shape[2]
    pad_length = 2 * cell_count
    plane_count = lax.axis_size("plane")
    band_width = pad_length // plane_count
    layer_index = lax.axis_index("layer")
    plane_index = lax.axis_index("plane")
    theta = polar[0]
    azimuthal = azimuth[0]
    moment_in = jnp.stack(
        [jnp.sin(theta) * jnp.cos(azimuthal), jnp.sin(theta) * jnp.sin(azimuthal), jnp.cos(theta)]
    )
    magnet = moment_in * saturation[0][None]
    place = jnp.arange(cell_count, dtype=jnp.int32)
    wave_index = jnp.arange(pad_length, dtype=jnp.int32)
    turns = place[:, None] * wave_index[None, :] % pad_length
    phase = turns.astype(jnp.float32) * (2.0 * jnp.pi / pad_length)
    cosine = jnp.cos(phase)
    sine = jnp.sin(phase)
    cosine_blocks = cosine.reshape(plane_count, row_count, pad_length)
    sine_blocks = sine.reshape(plane_count, row_count, pad_length)
    cosine_bands = cosine.reshape(cell_count, plane_count, band_width)
    sine_bands = sine.reshape(cell_count, plane_count, band_width)
    along_real = jnp.einsum("cxy,yk->ckx", magnet, cosine, precision=exact)
    along_imag = -jnp.einsum("cxy,yk->ckx", magnet, sine, precision=exact)
    sectioned = jnp.stack([along_real, along_imag], 1).reshape(
        3, 2, plane_count, band_width * row_count
    )
    block = lax.all_to_all(sectioned, "plane", split_axis=2, concat_axis=2, tiled=True)
    item_count = block.shape[0]
    split = block.reshape(item_count, 2, plane_count, band_width, row_count)
    with_cosine = jnp.einsum("npsqx,sxk->npqk", split, cosine_blocks, precision=exact)
    with_sine = jnp.einsum("npsqx,sxk->npqk", split, sine_blocks, precision=exact)
    spectrum = jnp.stack(
        [with_cosine[:, 0] + with_sine[:, 1], with_cosine[:, 1] - with_sine[:, 0]], 1
    )
    wave_y = signed_wave(
        plane_index * band_width + jnp.arange(band_width, dtype=jnp.int32), cell_count
    )[:, None]
    wave_x = signed_wave(wave_index, cell_count)[None, :]
    magnitude = jnp.sqrt(wave_x * wave_x + wave_y * wave_y)
    nonzero = magnitude > 0.0
    safe = jnp.where(nonzero, magnitude, 1.0)
    unit_x = jnp.where(nonzero, wave_x / safe, 0.0)
    unit_y = jnp.where(nonzero, wave_y / safe, 0.0)
    self_part = jnp.where(nonzero, -jnp.expm1(-safe) / safe, 1.0)
    half_sinh = jnp.sinh(0.5 * safe)
    mutual = jnp.where(nonzero, 2.0 * half_sinh * half_sinh / safe, 0.0)
    spectral_x = spectrum[0]
    spectral_y = spectrum[1]
    spectral_z = spectrum[2]
    inplane = unit_x * spectral_x + unit_y * spectral_y
    upward = jnp.stack([spectral_z[0] + inplane[1], spectral_z[1] - inplane[0]])
    downward = jnp.stack([-spectral_z[0] + inplane[1], -spectral_z[1] - inplane[0]])
    emitted = jnp.stack([upward, downward])[None]
    piece = lax.all_gather(emitted, "layer", axis=0, tiled=True)
    source = jnp.arange(piece.shape[0], dtype=jnp.int32)
    separation = layer_index - source
    distance = jnp.abs(separation).astype(jnp.float32)
    weight = jnp.exp(-spacing * distance[:, None, None] * magnitude[None])
    lower = jnp.where((separation > 0)[:, None, None], weight, 0.0)
    upper = jnp.where((separation < 0)[:, None, None], weight, 0.0)
    below = jnp.sum(lower[:, None] * piece[:, 0], 0)
    above = jnp.sum(upper[:, None] * piece[:, 1], 0)
    total = below + above
    differ = below - above
    remainder = 1.0 - self_part
    field_x = jnp.stack(
        [
            -remainder * unit_x * inplane[0] + unit_x * mutual * total[1],
            -remainder * unit_x * inplane[1] - unit_x * mutual * total[0],
        ]
    )
    field_y = jnp.stack(
        [
            -remainder * unit_y * inplane[0] + unit_y * mutual * total[1],
            -remainder * unit_y * inplane[1] - unit_y * mutual * total[0],
        ]
    )
    field_z = jnp.stack(
        [
            -self_part * spectral_z[0] + mutual * differ[0],
            -self_part * spectral_z[1] + mutual * differ[1],
        ]
    )
    spectral = jnp.stack([field_x, field_y, field_z])
    back_cosine = jnp.einsum("cpqk,sxk->cpsqx", spectral, cosine_blocks, precision=exact)
    back_sine = jnp.einsum("cpqk,sxk->cpsqx", spectral, sine_blocks, precision=exact)
    returned = jnp.stack(
        [back_cosine[:, 0] - back_sine[:, 1], back_sine[:, 0] + back_cosine[:, 1]], 1
    )
    returned = returned.reshape(3, 2, plane_count, band_width * row_count)
    scale = 1.0 / (float(pad_length) * float(pad_length))
    block = lax.all_to_all(returned, "plane", split_axis=2, concat_axis=2, tiled=True)
    item_count = block.shape[0]
    split = block.reshape(item_count, 2, plane_count, band_width, row_count)
    real_part = jnp.einsum("nsqx,ysq->nxy", split[:, 0], cosine_bands, precision=exact)
    imag_part = jnp.einsum("nsqx,ysq->nxy", split[:, 1], sine_bands, precision=exact)
    demag = (real_part - imag_part) * scale
    padded = with_halo(moment_in[None], (("layer", 0), ("plane", 2)), 1)
    centre = padded[1]
    beside = centre[:, :-2] + centre[:, 2:]
    sideways = jnp.pad(moment_in, ((0, 0), (0, 0), (1, 1)))
    beside = beside + sideways[:, :, :-2] + sideways[:, :, 2:]
    lower_link = coupling[jnp.maximum(layer_index - 1, 0)]
    upper_link = coupling[jnp.minimum(layer_index, coupling.shape[0] - 1)]
    exchange_field = (
        stiffness[0] * beside + lower_link * padded[0, :, 1:-1] + upper_link * padded[2, :, 1:-1]
    )
    flat_zero = jnp.zeros_like(moment_in[2])
    uniaxial = jnp.stack([flat_zero, flat_zero, anisotropy[0] * moment_in[2]])
    field = demag + exchange_field + uniaxial
    first_cross = cross_product(moment_in, field)
    second_cross = cross_product(moment_in, first_cross)
    torque = -(first_cross + damping * second_cross) / (1.0 + damping * damping)
    stepped = moment_in + time_step * torque
    length = jnp.sqrt(jnp.sum(stepped * stepped, axis=0, keepdims=True))
    return (field[None], (stepped / length)[None])


def body(polar, azimuth, saturation, anisotropy, stiffness, coupling):
    rows, cell_count = polar.shape[1:]
    device_count = lax.axis_size("layer") * lax.axis_size("plane")
    fits = 2 * rows == lanes and cell_count == 4 * lanes
    fits = fits and cell_count % (device_count * sublanes) == 0
    chosen = fast_body if fits else plain_body
    return chosen(polar, azimuth, saturation, anisotropy, stiffness, coupling)


def solution(mesh):
    placed = (
        P("layer", "plane", None),
        P("layer", "plane", None),
        P("layer", "plane", None),
        P("layer", "plane", None),
        P("layer"),
        P(),
    )
    return jax.shard_map(
        body,
        mesh=mesh,
        in_specs=placed,
        out_specs=(P("layer", None, "plane", None), P("layer", None, "plane", None)),
        check_vma=False,
    )
```

```python
import functools
import math

import jax
import jax.numpy as jnp
import numpy as np
from jax import lax
from jax.experimental import pallas as pl
from jax.experimental.pallas import tpu as pltpu
from jax.sharding import PartitionSpec as P


side_length = 512.0
spacing = 1.2
damping = 0.1
time_step = 0.1
exact = lax.Precision.HIGHEST

lanes = 128
sublanes = 8
half = lanes // 2
root_half = math.sqrt(0.5)
piece_count = 2
coef_count = 6
vmem_limit = 16 << 20
both = ("plane", "layer")
in_vmem = pl.BlockSpec(memory_space=pltpu.VMEM)
in_any = pl.BlockSpec(memory_space=pl.ANY)
in_smem = pl.BlockSpec(memory_space=pltpu.SMEM)


def split_table(table):
    head = table.astype(np.float32).astype(jnp.bfloat16)
    rest = (table - head.astype(np.float64)).astype(np.float32).astype(jnp.bfloat16)
    return np.stack([head, rest])


def edge_table():
    slot, place = np.arange(half), np.arange(lanes)
    zero = np.zeros((half, lanes))
    phase = [2.0 * np.pi / (8 * lanes) * (np.outer(8 * slot + r, place) % (8 * lanes)) for r in (0, 4)]
    rows = [np.block([[f(phase[0]), zero], [zero, f(phase[1])]]) for f in (np.cos, np.sin)]
    return split_table(np.concatenate([rows[0], -rows[1]]))


def short_table():
    turns = np.outer(np.arange(lanes), np.arange(lanes)) % lanes
    phase = turns * (2.0 * np.pi / lanes)
    c, s = np.cos(phase), np.sin(phase)
    return split_table(np.block([[c, s], [-s, c]]))


def twiddle_table(radix):
    phase = np.outer(np.arange(radix), np.arange(lanes)) * (2.0 * np.pi / (radix * lanes))
    pair = np.stack([np.cos(phase), np.sin(phase)]).astype(np.float32)
    return np.ascontiguousarray(np.broadcast_to(pair[:, :, None], (2, radix, sublanes, lanes)))


def split(value):
    head = value.astype(jnp.bfloat16)
    return head, (value - head.astype(jnp.float32)).astype(jnp.bfloat16)


def product(left, right, dims):
    (axis,), (other,) = dims
    return lax.dot_general(
        jnp.concatenate([left[0], left[1], left[0]], axis=axis),
        jnp.concatenate([right[0], right[0], right[1]], axis=other),
        dimension_numbers=(dims, ((), ())),
        preferred_element_type=jnp.float32,
    )


def sine_cosine(angle):
    square = angle * angle
    sine = jnp.full_like(angle, 1.0 / math.factorial(13))
    for order in (11, 9, 7, 5, 3, 1):
        sine = (-1.0) ** ((order - 1) // 2) / math.factorial(order) + square * sine
    cosine = jnp.full_like(angle, -1.0 / math.factorial(14))
    for order in (12, 10, 8, 6, 4, 2, 0):
        cosine = (-1.0) ** (order // 2) / math.factorial(order) + square * cosine
    return angle * sine, cosine


def first_kernel(
    polar_hbm, azimuth_hbm, saturation_hbm, edge_hbm, back_hbm, twiddle_hbm, moment_hbm, side_hbm, out_hbm,
    angle_ref, edge_ref, back_ref, twiddle_ref, moment_ref, side_ref, rows_ref, in_sem, out_sem,
):
    rows, _ = angle_ref.shape[1:]
    sources = (polar_hbm, azimuth_hbm, saturation_hbm, edge_hbm, back_hbm, twiddle_hbm)
    places = (angle_ref.at[0], angle_ref.at[1], angle_ref.at[2], edge_ref, back_ref, twiddle_ref)
    loads = [
        pltpu.make_async_copy(source, place, in_sem.at[n])
        for n, (source, place) in enumerate(zip(sources, places))
    ]
    for copy in loads:
        copy.start()
    for copy in loads[:3]:
        copy.wait()
    sin_polar, cos_polar = sine_cosine(angle_ref[0])
    sin_half, cos_half = sine_cosine(0.5 * angle_ref[1])
    saturation = angle_ref[2]
    moment = (
        sin_polar * (1.0 - 2.0 * sin_half * sin_half),
        sin_polar * (2.0 * sin_half * cos_half),
        cos_polar,
    )
    for copy in loads[3:]:
        copy.wait()
    groups = [[] for _ in range(4)]
    for c in range(3):
        moment_ref[c] = moment[c]
        side_ref[0, c : c + 1] = moment[c][:1]
        side_ref[1, c : c + 1] = moment[c][rows - 1 :]
        magnet = moment[c] * saturation
        a = [magnet[:, p * lanes : (p + 1) * lanes] for p in range(4)]
        even, odd = a[0] + a[2], a[1] + a[3]
        turned, mixed = root_half * (a[1] - a[3]), root_half * odd
        groups[0].append((even + odd, even - odd))
        for r, (real, imag) in (
            (1, (a[0] + turned, -a[2] - mixed)),
            (2, (a[0] - a[2], a[3] - a[1])),
            (3, (a[0] - turned, a[2] - mixed)),
        ):
            cosine, sine = twiddle_ref[0, r, :1], twiddle_ref[1, r, :1]
            groups[r].append((real * cosine + imag * sine, imag * cosine - real * sine))
    sends = [
        pltpu.make_async_copy(moment_ref, moment_hbm, out_sem.at[0]),
        pltpu.make_async_copy(side_ref, side_hbm, out_sem.at[1]),
    ]
    for copy in sends:
        copy.start()
    blank = jnp.zeros((rows, 2 * lanes), jnp.bfloat16)
    dims = ((1,), (1,))
    for g in range(4):
        parts = [split(jnp.concatenate(pair, axis=1)) for pair in groups[g]]
        for_real = [jnp.concatenate([part[n] for part in parts] + [blank]) for n in range(2)]
        for_imag = [jnp.concatenate([blank] + [part[n] for part in parts]) for n in range(2)]
        table_ref = edge_ref if g == 0 else back_ref
        real = product((table_ref[0, :lanes], table_ref[1, :lanes]), for_real, dims)
        imag = product((table_ref[0, lanes:], table_ref[1, lanes:]), for_imag, dims)
        cut = slice(g * lanes, (g + 1) * lanes)
        rows_ref[cut, :lanes] = real[:, :lanes]
        rows_ref[cut, lanes : 2 * lanes] = real[:, lanes:] + imag[:, :lanes]
        rows_ref[cut, 2 * lanes :] = imag[:, lanes:]
        sends.append(pltpu.make_async_copy(rows_ref.at[cut], out_hbm.at[cut], out_sem.at[2 + g]))
        sends[-1].start()
    for copy in sends:
        copy.wait()


def factors(wave_x, wave_y):
    magnitude = jnp.sqrt(wave_x * wave_x + wave_y * wave_y)
    nonzero = magnitude > 0.0
    safe = jnp.where(nonzero, magnitude, 1.0)
    inverse = 1.0 / safe
    series = jnp.ones_like(safe)
    for order in range(9, 1, -1):
        series = 1.0 - series * safe * (1.0 / order)
    growth = jnp.exp(safe)
    lost = jnp.where(safe < 0.5, series * safe, 1.0 - jnp.exp(-safe))
    self_part = jnp.where(nonzero, lost * inverse, 1.0)
    mutual = jnp.where(nonzero, lost * lost * growth * (0.5 * inverse), 0.0)
    decay = jnp.exp(-spacing * magnitude)
    unit_x = jnp.where(nonzero, wave_x * inverse, 0.0)
    unit_y = jnp.where(nonzero, wave_y * inverse, 0.0)
    return unit_x, unit_y, self_part, mutual, decay


def coef_kernel(base_ref, *refs, cell_count):
    count = len(refs) // 2 - 1
    out_ref, edge_ref, sign_ref = refs[count : count + 3]
    for table_ref, kept_ref in zip(refs[:count], refs[count + 3 :]):
        kept_ref[...] = table_ref[...]
    pad_length = 2 * cell_count
    radix = pad_length // lanes
    step = math.pi / side_length
    slots = out_ref.shape[2]
    shape = (slots, lanes)
    slot = base_ref[0] * slots + lax.broadcasted_iota(jnp.int32, shape, 0)
    group, order = slot // lanes, slot % lanes
    first = jnp.where(order < half, order * radix, (order - half) * radix + radix // 2)
    wave = jnp.where(group == 0, first, order * radix + group)
    wave_y = step * jnp.where(wave < cell_count, wave, wave - pad_length).astype(jnp.float32)
    weight = jnp.where(wave == 0, 1.0, 2.0) / float(pad_length * pad_length)
    sign_ref[...] = jnp.where(wave % 2 == 0, weight, -weight)
    for r in range(radix):
        index = lax.broadcasted_iota(jnp.int32, shape, 1) * radix + r
        folded = jnp.where(index < cell_count, index, index - pad_length)
        unit_x, unit_y, self_part, mutual, decay = factors(step * folded.astype(jnp.float32), wave_y)
        out_ref[0, r] = jnp.where(index == cell_count, 0.0, unit_x)
        out_ref[1, r] = unit_y
        out_ref[2, r] = (1.0 - self_part) * weight
        out_ref[3, r] = self_part * weight
        out_ref[4, r] = mutual * weight
        out_ref[5, r] = decay
    shape = (radix, lanes)
    index = lax.broadcasted_iota(jnp.int32, shape, 1) * radix + lax.broadcasted_iota(jnp.int32, shape, 0)
    folded = jnp.where(index < cell_count, index, index - pad_length)
    wave_y = jnp.full(shape, -step * cell_count, jnp.float32)
    edge_x, edge_y, self_part, mutual, decay = factors(step * folded.astype(jnp.float32), wave_y)
    edge_ref[0] = jnp.where(index == cell_count, 0.0, edge_x)
    edge_ref[1] = 1.0 - self_part
    edge_ref[2] = self_part
    edge_ref[3] = mutual
    edge_ref[4] = decay
    edge_ref[5] = edge_y * edge_y


def neighbours(values, decay):
    count = len(values)
    under = [None] * count
    over = [None] * count
    for t in range(1, count):
        under[t] = decay * (values[t - 1] if under[t - 1] is None else under[t - 1] + values[t - 1])
    for t in range(count - 2, -1, -1):
        over[t] = decay * (values[t + 1] if over[t + 1] is None else over[t + 1] + values[t + 1])
    return under, over


def joined(first, second, sign=1.0):
    if first is None:
        return second if sign > 0.0 else -second
    if second is None:
        return first
    return first + second if sign > 0.0 else first - second


def drive(x, z, keep, mutual, decay, own):
    count = len(x)
    up_r, over_r = [z[t][0] + x[t][1] for t in range(count)], [x[t][1] - z[t][0] for t in range(count)]
    up_i, over_i = [z[t][1] - x[t][0] for t in range(count)], [-z[t][1] - x[t][0] for t in range(count)]
    below_r, below_i = neighbours(up_r, decay)[0], neighbours(up_i, decay)[0]
    above_r, above_i = neighbours(over_r, decay)[1], neighbours(over_i, decay)[1]
    inner, outer = [], []
    for t in range(count):
        total_r, total_i = joined(below_r[t], above_r[t]), joined(below_i[t], above_i[t])
        differ_r = joined(below_r[t], above_r[t], -1.0)
        differ_i = joined(below_i[t], above_i[t], -1.0)
        inner.append((mutual * total_i - keep * x[t][0], -(mutual * total_r) - keep * x[t][1]))
        outer.append((mutual * differ_r - own * z[t][0], mutual * differ_i - own * z[t][1]))
    return inner, outer


def even_part(values, keep, mutual, decay):
    out = []
    for n in range(2):
        part = [v[n] for v in values]
        under, over = neighbours(part, decay)
        out.append([-(keep * part[t]) - mutual * joined(under[t], over[t]) for t in range(len(part))])
    return list(zip(*out))


def respond(spectrum, coef, has_middle, middle):
    count = len(spectrum)
    unit_x, unit_y, keep, own, mutual, decay = coef[:6]
    edge_x, edge_keep, edge_own, edge_mutual, edge_decay, square_y, sign = coef[6:]
    edge_keep, edge_own, edge_mutual = sign * edge_keep, sign * edge_own, sign * edge_mutual
    keep_y, mutual_y = square_y * edge_keep, square_y * edge_mutual
    x = [s[0] for s in spectrum]
    y = [s[1] for s in spectrum]
    z = [s[2] for s in spectrum]
    charge = [tuple(unit_x * x[t][n] + unit_y * y[t][n] for n in range(2)) for t in range(count)]
    inner, outer = drive(charge, z, keep, mutual, decay, own)
    charge = [tuple(edge_x * x[t][n] for n in range(2)) for t in range(count)]
    edge_inner, edge_outer = drive(charge, z, edge_keep, edge_mutual, edge_decay, edge_own)
    edge_y = even_part(y, keep_y, mutual_y, edge_decay)
    out = []
    for t in range(count):
        out.append(
            [
                tuple(unit_x * inner[t][n] - edge_x * edge_inner[t][n] for n in range(2)),
                tuple(unit_y * inner[t][n] - edge_y[t][n] for n in range(2)),
                tuple(outer[t][n] - edge_outer[t][n] for n in range(2)),
            ]
        )
    if has_middle:
        square = jnp.where(middle, 1.0 - unit_y * unit_y, 0.0)
        alone = even_part(x, keep * square, mutual * square, decay)
        keep_m, mutual_m = jnp.where(middle, keep_y, 0.0), jnp.where(middle, mutual_y, 0.0)
        cross_x = even_part(x, keep_m, mutual_m, edge_decay)
        cross_y = even_part(y, keep_m, mutual_m, edge_decay)
        for t in range(count):
            out[t][0] = tuple(
                out[t][0][n] + alone[t][n] - cross_x[t][n] - cross_y[t][n] for n in range(2)
            )
            out[t][1] = tuple(out[t][1][n] - cross_x[t][n] for n in range(2))
    return out


def add(a, b):
    return a[0] + b[0], a[1] + b[1]


def sub(a, b):
    return a[0] - b[0], a[1] - b[1]


def add_turned(a, b):
    return a[0] - b[1], a[1] + b[0]


def sub_turned(a, b):
    return a[0] + b[1], a[1] - b[0]


def four_point(z):
    s, d, u, v = add(z[0], z[2]), sub(z[0], z[2]), add(z[1], z[3]), sub(z[1], z[3])
    return add(s, u), sub_turned(d, v), sub(s, u), add_turned(d, v)


def four_point_back(z):
    s, d, u, v = add(z[0], z[2]), sub(z[0], z[2]), add(z[1], z[3]), sub(z[1], z[3])
    return add(s, u), add_turned(d, v), sub(s, u), sub_turned(d, v)


def spread(z):
    turned = [
        z[0],
        (root_half * (z[1][0] + z[1][1]), root_half * (z[1][1] - z[1][0])),
        (z[2][1], -z[2][0]),
        (root_half * (z[3][1] - z[3][0]), -root_half * (z[3][0] + z[3][1])),
    ]
    even, odd = four_point(z), four_point(turned)
    return [even[r // 2] if r % 2 == 0 else odd[r // 2] for r in range(8)]


def gather_back(v):
    even, odd = four_point_back(v[0::2]), four_point_back(v[1::2])
    return [
        add(even[0], odd[0]),
        (even[1][0] + root_half * (odd[1][0] - odd[1][1]), even[1][1] + root_half * (odd[1][0] + odd[1][1])),
        add_turned(even[2], odd[2]),
        (even[3][0] - root_half * (odd[3][0] + odd[3][1]), even[3][1] + root_half * (odd[3][0] - odd[3][1])),
    ]


def middle_kernel(
    rows_ref, coef_ref, edge_ref, sign_ref, twiddle_ref, back_ref, out_ref, work_ref, *, layers
):
    radix = twiddle_ref.shape[1]
    pieces = radix // 2
    steps = rows_ref.shape[1] // sublanes
    items = layers * 3
    place = lax.broadcasted_iota(jnp.int32, (sublanes, lanes), 1)
    low = place < half
    dims = ((1,), (0,))
    back = (back_ref[0], back_ref[1])
    upper = [jnp.concatenate([b[:lanes, :lanes], b[lanes:, :lanes]], axis=1) for b in back]
    lower = [jnp.concatenate([b[:lanes, lanes:], b[lanes:, lanes:]], axis=1) for b in back]
    forward = tuple(jnp.concatenate(pair) for pair in zip(upper, lower))

    def run(step):
        here = slice(step * sublanes, (step + 1) * sublanes)

        def piece(row, part):
            tile, upper = divmod(part, 2)
            cut = slice(tile * lanes, (tile + 1) * lanes)
            first, second = rows_ref[row, here, cut], rows_ref[row + layers, here, cut]
            if upper:
                return jnp.where(low, pltpu.roll(first, half, 1), second)
            return jnp.where(low, first, pltpu.roll(second, half, 1))

        for item in range(items):
            layer, c = divmod(item, 3)
            rows = [2 * p * layers + layer for p in range(pieces)]
            z = [(piece(row, c), piece(row, 3 + c)) for row in rows]
            for r, (real, imag) in enumerate(spread(z)):
                if r > 0:
                    cosine, sine = twiddle_ref[0, r], twiddle_ref[1, r]
                    real, imag = real * cosine + imag * sine, imag * cosine - real * sine
                start = item * sublanes
                work_ref[step, r, start : start + sublanes, :lanes] = real
                work_ref[step, r, start : start + sublanes, lanes:] = imag
        for r in range(radix):
            work_ref[step, r] = product(split(work_ref[step, r]), forward, dims)
        for r in range(radix):
            value = work_ref[step, r]
            cuts = [slice(item * sublanes, (item + 1) * sublanes) for item in range(items)]
            pairs = [(value[cut, :lanes], value[cut, lanes:]) for cut in cuts]
            spectrum = [pairs[3 * t : 3 * t + 3] for t in range(layers)]
            coef = [coef_ref[n, r, here] for n in range(coef_count)]
            coef += [edge_ref[n, r : r + 1] for n in range(coef_count)] + [sign_ref[here]]
            out = respond(spectrum, coef, r == 0, place * radix + r == radix * half)
            work_ref[step, r] = jnp.concatenate(
                [jnp.concatenate([pair[0], pair[1]], axis=1) for layer in out for pair in layer]
            )
        for r in range(radix):
            work_ref[step, r] = product(split(work_ref[step, r]), back, dims)
        for layer in range(layers):
            parts = [[None] * 6 for _ in range(pieces)]
            for c in range(3):
                start = (layer * 3 + c) * sublanes
                v = []
                for r in range(radix):
                    real = work_ref[step, r, start : start + sublanes, :lanes]
                    imag = work_ref[step, r, start : start + sublanes, lanes:]
                    if r > 0:
                        cosine, sine = twiddle_ref[0, r], twiddle_ref[1, r]
                        real, imag = real * cosine - imag * sine, imag * cosine + real * sine
                    v.append((real, imag))
                for p, (real, imag) in enumerate(gather_back(v)):
                    parts[p][c], parts[p][3 + c] = real, imag
            for p in range(pieces):
                row = 2 * p * layers + layer
                for tile in range(3):
                    first, second = parts[p][2 * tile], parts[p][2 * tile + 1]
                    cut = slice(tile * lanes, (tile + 1) * lanes)
                    out_ref[row, here, cut] = jnp.where(low, first, pltpu.roll(second, half, 1))
                    out_ref[row + layers, here, cut] = jnp.where(low, pltpu.roll(first, half, 1), second)

    for step in range(steps):
        run(step)


def exchange_kernel(place_ref, stiffness_ref, coupling_ref, moment_ref, below_ref, above_ref, anisotropy_ref, out_ref, scale_ref):
    scale_ref[...] = jnp.full_like(scale_ref, stiffness_ref[0])
    rows, cell_count = anisotropy_ref.shape
    row = lax.broadcasted_iota(jnp.int32, (rows, cell_count), 0)
    column = lax.broadcasted_iota(jnp.int32, (rows, cell_count), 1)
    stiffness = stiffness_ref[0]
    lower_link = coupling_ref[jnp.maximum(place_ref[1] - 1, 0)]
    upper_link = coupling_ref[jnp.minimum(place_ref[1], coupling_ref.shape[0] - 1)]
    for c in range(3):
        m = moment_ref[c]
        before = jnp.where(row == 0, 0.0, pltpu.roll(m, 1, 0))
        after = jnp.where(row == rows - 1, 0.0, pltpu.roll(m, rows - 1, 0))
        left = jnp.where(column == 0, 0.0, pltpu.roll(m, 1, 1))
        right = jnp.where(column == cell_count - 1, 0.0, pltpu.roll(m, cell_count - 1, 1))
        total = stiffness * (before + after + left + right)
        total = total + lower_link * below_ref[c] + upper_link * above_ref[c]
        if c == 2:
            total = total + anisotropy_ref[...] * m
        out_ref[c] = total


def last_kernel(
    before_any, after_any, scale_any, moment_ref, other_ref, edge_ref, back_ref, twiddle_ref, block_ref,
    field_hbm, out_hbm, field_ref, out_ref, side_ref, field_sem, out_sem, side_sem,
):
    rows = moment_ref.shape[1]
    sides = [
        pltpu.make_async_copy(source, side_ref.at[n], side_sem.at[n])
        for n, source in enumerate((before_any, after_any, scale_any))
    ]
    for copy in sides:
        copy.start()
    turned = block_ref[...].T
    dims = ((1,), (0,))
    waves = []
    for g in range(4):
        cut = slice(g * lanes, (g + 1) * lanes)
        value = jnp.concatenate([turned[: 3 * rows, cut], turned[3 * rows :, cut]], axis=1)
        table_ref = edge_ref if g == 0 else back_ref
        value = product(split(value), (table_ref[0], table_ref[1]), dims)
        real, imag = value[:, :lanes], value[:, lanes:]
        if g > 0:
            cosine, sine = twiddle_ref[0, g, :1], twiddle_ref[1, g, :1]
            real, imag = real * cosine - imag * sine, imag * cosine + real * sine
        waves.append((real, imag))
    even, odd = waves[0][0] + waves[0][1], waves[0][0] - waves[0][1]
    (real_1, imag_1), (real_2, imag_2), (real_3, imag_3) = waves[1:]
    flat, tilted = root_half * (real_1 - real_3), root_half * (imag_1 + imag_3)
    demag = jnp.concatenate(
        [
            even + real_1 + real_2 + real_3,
            odd + flat - tilted - imag_2,
            even - imag_1 - real_2 + imag_3,
            odd - flat - tilted + imag_2,
        ],
        axis=1,
    )
    for copy in sides:
        copy.wait()
    for c in range(3):
        field_ref[c] = other_ref[c] + demag[c * rows : (c + 1) * rows]
        field_ref[c, :1] += side_ref[2, :1] * side_ref[0, c : c + 1]
        field_ref[c, rows - 1 :] += side_ref[2, :1] * side_ref[1, c : c + 1]
    sends = [pltpu.make_async_copy(field_ref, field_hbm, field_sem)]
    sends[0].start()
    span = rows // piece_count
    for n in range(piece_count):
        cut = pl.ds(n * span, span)
        m = [moment_ref[c, cut] for c in range(3)]
        first = cross(m, [field_ref[c, cut] for c in range(3)])
        second = cross(m, first)
        stepped = []
        for c in range(3):
            torque = -(first[c] + damping * second[c]) / (1.0 + damping * damping)
            stepped.append(m[c] + time_step * torque)
        scale = lax.rsqrt(stepped[0] * stepped[0] + stepped[1] * stepped[1] + stepped[2] * stepped[2])
        for c in range(3):
            out_ref[c, cut] = stepped[c] * scale
        sends.append(pltpu.make_async_copy(out_ref.at[:, cut], out_hbm.at[:, cut], out_sem.at[n]))
        sends[-1].start()
    for copy in sends:
        copy.wait()


def cross(first, second):
    return [
        first[1] * second[2] - first[2] * second[1],
        first[2] * second[0] - first[0] * second[2],
        first[0] * second[1] - first[1] * second[0],
    ]


def shift(value, axis, step):
    count = lax.axis_size(axis)
    pairs = [(i, i + step) for i in range(count) if 0 <= i + step < count]
    return lax.ppermute(value, axis, pairs)


def fast_body(polar, azimuth, saturation, anisotropy, stiffness, coupling):
    rows, cell_count = polar.shape[1:]
    layers, planes = lax.axis_size("layer"), lax.axis_size("plane")
    device_count = layers * planes
    layer_index = lax.axis_index("layer")
    plane_index = lax.axis_index("plane")
    slots = cell_count // device_count
    radix = 2 * cell_count // lanes
    width = 6 * rows
    f32, bf16 = jnp.float32, jnp.bfloat16
    edge = jnp.asarray(edge_table())
    back = jnp.asarray(short_table())
    twiddle = jnp.asarray(twiddle_table(radix))
    field_shape = jax.ShapeDtypeStruct((3, rows, cell_count), f32)
    side_shape = (2, sublanes, cell_count)
    block_shape = jax.ShapeDtypeStruct((cell_count, width), f32)
    small = pltpu.CompilerParams(vmem_limit_bytes=vmem_limit)
    dma = pltpu.SemaphoreType.DMA
    flops = 12 * rows * cell_count * cell_count * 6

    moment, side, block = pl.pallas_call(
        first_kernel,
        out_shape=[field_shape, jax.ShapeDtypeStruct(side_shape, f32), block_shape],
        in_specs=[in_any] * 6,
        out_specs=[in_any] * 3,
        scratch_shapes=[
            pltpu.VMEM((3, rows, cell_count), f32),
            pltpu.VMEM(edge.shape, bf16),
            pltpu.VMEM(back.shape, bf16),
            pltpu.VMEM(twiddle.shape, f32),
            pltpu.VMEM((3, rows, cell_count), f32),
            pltpu.VMEM(side_shape, f32),
            pltpu.VMEM((cell_count, width), f32),
            dma((6,)),
            dma((6,)),
        ],
        cost_estimate=pl.CostEstimate(flops=flops, bytes_accessed=4 << 20, transcendentals=0),
        name="first",
    )(polar[0], azimuth[0], saturation[0], edge, back, twiddle)

    base = jnp.stack([plane_index * layers + layer_index, layer_index]).astype(jnp.int32)
    tables = (twiddle, back)
    *coefs, kept_twiddle, kept_back = pl.pallas_call(
        functools.partial(coef_kernel, cell_count=cell_count),
        out_shape=[
            jax.ShapeDtypeStruct((coef_count, radix, slots, lanes), f32),
            jax.ShapeDtypeStruct((coef_count, radix, lanes), f32),
            jax.ShapeDtypeStruct((slots, lanes), f32),
        ]
        + [jax.ShapeDtypeStruct(t.shape, t.dtype) for t in tables],
        in_specs=[in_smem] + [in_vmem] * len(tables),
        out_specs=[in_vmem] * (3 + len(tables)),
        compiler_params=small,
        cost_estimate=pl.CostEstimate(flops=20 << 20, bytes_accessed=1 << 20, transcendentals=1 << 16),
        name="coefs",
    )(base, *tables)

    below = shift(moment, "layer", 1)
    above = shift(moment, "layer", -1)
    before = shift(side[1], "plane", 1)
    after = shift(side[0], "plane", -1)
    other, scale = pl.pallas_call(
        exchange_kernel,
        out_shape=[field_shape, jax.ShapeDtypeStruct(side_shape[1:], f32)],
        in_specs=[in_smem] * 3 + [in_vmem] * 4,
        out_specs=[in_vmem] * 2,
        compiler_params=small,
        cost_estimate=pl.CostEstimate(flops=20 << 20, bytes_accessed=2 << 20, transcendentals=0),
        name="exchange",
    )(base, stiffness, coupling, moment, below, above, anisotropy[0])

    exchange_all = functools.partial(
        lax.all_to_all, axis_name=both, split_axis=0, concat_axis=0, tiled=True
    )
    block = exchange_all(block.reshape(device_count, slots, width))
    block, other = lax.optimization_barrier((block, other))
    block = pl.pallas_call(
        functools.partial(middle_kernel, layers=layers),
        out_shape=jax.ShapeDtypeStruct((device_count, slots, width), f32),
        in_specs=[in_vmem] * 6,
        out_specs=in_vmem,
        scratch_shapes=[pltpu.VMEM((slots // sublanes, radix, layers * 3 * sublanes, 2 * lanes), f32)],
        compiler_params=small,
        cost_estimate=pl.CostEstimate(flops=2000 << 20, bytes_accessed=4 << 20, transcendentals=0),
        name="middle",
    )(block, *coefs, kept_twiddle, kept_back)
    block, before, after = lax.optimization_barrier((block, before, after))
    block = exchange_all(block)

    field, stepped = pl.pallas_call(
        last_kernel,
        out_shape=[field_shape] * 2,
        in_specs=[in_any] * 3 + [in_vmem] * 6,
        out_specs=[in_any] * 2,
        scratch_shapes=[
            pltpu.VMEM((3, rows, cell_count), f32),
            pltpu.VMEM((3, rows, cell_count), f32),
            pltpu.VMEM((3, *side_shape[1:]), f32),
            dma,
            dma((piece_count,)),
            dma((3,)),
        ],
        compiler_params=small,
        cost_estimate=pl.CostEstimate(flops=flops, bytes_accessed=4 << 20, transcendentals=0),
        name="last",
    )(before, after, scale, moment, other, edge, back, twiddle, block.reshape(cell_count, width))
    return field[None], stepped[None]


def with_halo(cells, sides, width):
    for axis, dim in sides:
        count = lax.axis_size(axis)
        ends = count - 1
        head = lax.slice_in_dim(cells, 0, width, axis=dim)
        tail = lax.slice_in_dim(cells, cells.shape[dim] - width, cells.shape[dim], axis=dim)
        cells = jnp.concatenate(
            [
                lax.ppermute(tail, axis, [(i, (i + 1) % count) for i in range(ends)]),
                cells,
                lax.ppermute(head, axis, [((i + 1) % count, i) for i in range(ends)]),
            ],
            axis=dim,
        )
    return cells


def cross_product(first, second):
    return jnp.stack(
        [
            first[1] * second[2] - first[2] * second[1],
            first[2] * second[0] - first[0] * second[2],
            first[0] * second[1] - first[1] * second[0],
        ]
    )


def signed_wave(index, cell_count):
    folded = jnp.where(index < cell_count, index, index - 2 * cell_count)
    return jnp.pi * folded.astype(jnp.float32) / side_length


def plain_body(polar, azimuth, saturation, anisotropy, stiffness, coupling):
    row_count = polar.shape[1]
    cell_count = polar.shape[2]
    pad_length = 2 * cell_count
    plane_count = lax.axis_size("plane")
    band_width = pad_length // plane_count
    layer_index = lax.axis_index("layer")
    plane_index = lax.axis_index("plane")
    theta = polar[0]
    azimuthal = azimuth[0]
    moment_in = jnp.stack(
        [jnp.sin(theta) * jnp.cos(azimuthal), jnp.sin(theta) * jnp.sin(azimuthal), jnp.cos(theta)]
    )
    magnet = moment_in * saturation[0][None]
    place = jnp.arange(cell_count, dtype=jnp.int32)
    wave_index = jnp.arange(pad_length, dtype=jnp.int32)
    turns = place[:, None] * wave_index[None, :] % pad_length
    phase = turns.astype(jnp.float32) * (2.0 * jnp.pi / pad_length)
    cosine = jnp.cos(phase)
    sine = jnp.sin(phase)
    cosine_blocks = cosine.reshape(plane_count, row_count, pad_length)
    sine_blocks = sine.reshape(plane_count, row_count, pad_length)
    cosine_bands = cosine.reshape(cell_count, plane_count, band_width)
    sine_bands = sine.reshape(cell_count, plane_count, band_width)
    along_real = jnp.einsum("cxy,yk->ckx", magnet, cosine, precision=exact)
    along_imag = -jnp.einsum("cxy,yk->ckx", magnet, sine, precision=exact)
    sectioned = jnp.stack([along_real, along_imag], 1).reshape(
        3, 2, plane_count, band_width * row_count
    )
    block = lax.all_to_all(sectioned, "plane", split_axis=2, concat_axis=2, tiled=True)
    item_count = block.shape[0]
    split = block.reshape(item_count, 2, plane_count, band_width, row_count)
    with_cosine = jnp.einsum("npsqx,sxk->npqk", split, cosine_blocks, precision=exact)
    with_sine = jnp.einsum("npsqx,sxk->npqk", split, sine_blocks, precision=exact)
    spectrum = jnp.stack(
        [with_cosine[:, 0] + with_sine[:, 1], with_cosine[:, 1] - with_sine[:, 0]], 1
    )
    wave_y = signed_wave(
        plane_index * band_width + jnp.arange(band_width, dtype=jnp.int32), cell_count
    )[:, None]
    wave_x = signed_wave(wave_index, cell_count)[None, :]
    magnitude = jnp.sqrt(wave_x * wave_x + wave_y * wave_y)
    nonzero = magnitude > 0.0
    safe = jnp.where(nonzero, magnitude, 1.0)
    unit_x = jnp.where(nonzero, wave_x / safe, 0.0)
    unit_y = jnp.where(nonzero, wave_y / safe, 0.0)
    self_part = jnp.where(nonzero, -jnp.expm1(-safe) / safe, 1.0)
    half_sinh = jnp.sinh(0.5 * safe)
    mutual = jnp.where(nonzero, 2.0 * half_sinh * half_sinh / safe, 0.0)
    spectral_x = spectrum[0]
    spectral_y = spectrum[1]
    spectral_z = spectrum[2]
    inplane = unit_x * spectral_x + unit_y * spectral_y
    upward = jnp.stack([spectral_z[0] + inplane[1], spectral_z[1] - inplane[0]])
    downward = jnp.stack([-spectral_z[0] + inplane[1], -spectral_z[1] - inplane[0]])
    emitted = jnp.stack([upward, downward])[None]
    piece = lax.all_gather(emitted, "layer", axis=0, tiled=True)
    source = jnp.arange(piece.shape[0], dtype=jnp.int32)
    separation = layer_index - source
    distance = jnp.abs(separation).astype(jnp.float32)
    weight = jnp.exp(-spacing * distance[:, None, None] * magnitude[None])
    lower = jnp.where((separation > 0)[:, None, None], weight, 0.0)
    upper = jnp.where((separation < 0)[:, None, None], weight, 0.0)
    below = jnp.sum(lower[:, None] * piece[:, 0], 0)
    above = jnp.sum(upper[:, None] * piece[:, 1], 0)
    total = below + above
    differ = below - above
    remainder = 1.0 - self_part
    field_x = jnp.stack(
        [
            -remainder * unit_x * inplane[0] + unit_x * mutual * total[1],
            -remainder * unit_x * inplane[1] - unit_x * mutual * total[0],
        ]
    )
    field_y = jnp.stack(
        [
            -remainder * unit_y * inplane[0] + unit_y * mutual * total[1],
            -remainder * unit_y * inplane[1] - unit_y * mutual * total[0],
        ]
    )
    field_z = jnp.stack(
        [
            -self_part * spectral_z[0] + mutual * differ[0],
            -self_part * spectral_z[1] + mutual * differ[1],
        ]
    )
    spectral = jnp.stack([field_x, field_y, field_z])
    back_cosine = jnp.einsum("cpqk,sxk->cpsqx", spectral, cosine_blocks, precision=exact)
    back_sine = jnp.einsum("cpqk,sxk->cpsqx", spectral, sine_blocks, precision=exact)
    returned = jnp.stack(
        [back_cosine[:, 0] - back_sine[:, 1], back_sine[:, 0] + back_cosine[:, 1]], 1
    )
    returned = returned.reshape(3, 2, plane_count, band_width * row_count)
    scale = 1.0 / (float(pad_length) * float(pad_length))
    block = lax.all_to_all(returned, "plane", split_axis=2, concat_axis=2, tiled=True)
    item_count = block.shape[0]
    split = block.reshape(item_count, 2, plane_count, band_width, row_count)
    real_part = jnp.einsum("nsqx,ysq->nxy", split[:, 0], cosine_bands, precision=exact)
    imag_part = jnp.einsum("nsqx,ysq->nxy", split[:, 1], sine_bands, precision=exact)
    demag = (real_part - imag_part) * scale
    padded = with_halo(moment_in[None], (("layer", 0), ("plane", 2)), 1)
    centre = padded[1]
    beside = centre[:, :-2] + centre[:, 2:]
    sideways = jnp.pad(moment_in, ((0, 0), (0, 0), (1, 1)))
    beside = beside + sideways[:, :, :-2] + sideways[:, :, 2:]
    lower_link = coupling[jnp.maximum(layer_index - 1, 0)]
    upper_link = coupling[jnp.minimum(layer_index, coupling.shape[0] - 1)]
    exchange_field = (
        stiffness[0] * beside + lower_link * padded[0, :, 1:-1] + upper_link * padded[2, :, 1:-1]
    )
    flat_zero = jnp.zeros_like(moment_in[2])
    uniaxial = jnp.stack([flat_zero, flat_zero, anisotropy[0] * moment_in[2]])
    field = demag + exchange_field + uniaxial
    first_cross = cross_product(moment_in, field)
    second_cross = cross_product(moment_in, first_cross)
    torque = -(first_cross + damping * second_cross) / (1.0 + damping * damping)
    stepped = moment_in + time_step * torque
    length = jnp.sqrt(jnp.sum(stepped * stepped, axis=0, keepdims=True))
    return (field[None], (stepped / length)[None])


def body(polar, azimuth, saturation, anisotropy, stiffness, coupling):
    rows, cell_count = polar.shape[1:]
    device_count = lax.axis_size("layer") * lax.axis_size("plane")
    fits = 2 * rows == lanes and cell_count == 4 * lanes
    fits = fits and cell_count % (device_count * sublanes) == 0
    chosen = fast_body if fits else plain_body
    return chosen(polar, azimuth, saturation, anisotropy, stiffness, coupling)


def solution(mesh):
    placed = (
        P("layer", "plane", None),
        P("layer", "plane", None),
        P("layer", "plane", None),
        P("layer", "plane", None),
        P("layer"),
        P(),
    )
    return jax.shard_map(
        body,
        mesh=mesh,
        in_specs=placed,
        out_specs=(P("layer", None, "plane", None), P("layer", None, "plane", None)),
        check_vma=False,
    )
```
